128 devices in a mesh: gene: 8 (over x, z_lo), var: 8 (over y, core), perm: 2 (over z_hi).
Axes of the slice: x: 4, y: 4, z: 4 (z_hi: 2, z_lo: 2; z = z_hi * 2 + z_lo), core: 2. Of those that a mesh axis runs over, the one named last changes fastest.
Arguments:
- genotypes: bfloat16 [8, 6144, 768], P('gene', ('var', 'perm')), may hold values from 0 to 2
- phenotypes: float32 [1024, 768], P('gene'), may hold values from -6 to 6
- perm_rows: int32 [256, 768], P(('var', 'perm')), may hold values from 0 to 767, each once within a row
- starts: int32 [1024], P('gene'), may hold values from 0 to 2048, as said below
Outputs:
- maxima: float32 [256, 1024], P(('var', 'perm'), 'gene')
- moments: float32 [2, 1024], P(None, 'gene')
- pooled: float32 [2], replicated
The draws below stay inside these ranges and needn't reach their ends.
Inputs may be any that keep to these rules, and one draw needn't show every extreme that they name: `perm_rows`: each row is a permutation of 0 to 767. Within each block of 128 genes the starts never fall; a gene's window of 4096 variants lies inside its block's 6144 variants.
All inputs are finite; a program needn't handle non-finite values.
Results may differ from the reference program's by a relative error of at most 0.0023.
Values may be sent and summed in bfloat16 or wider, within the bound.
No kernel may reach another device: no remote copies, remote signals or barrier semaphores. Data moves between devices by JAX's collectives and lax.ppermute only.
A program may use at most 64 MiB of HBM per device.

```python
import math
import jax
import jax.numpy as jnp
from jax import lax

SAMPLES = 768
WINDOW = 4096
SPAN = 6144
PERMS = 256
BLOCK_GENES = 128
BLOCKS = 8
GENES = 1024


def draw_starts(key, part):
    drawn = jax.random.randint(key, (GENES,), 0, SPAN - WINDOW + 1, dtype=jnp.int32)
    return jnp.sort(drawn.reshape(GENES // BLOCK_GENES, BLOCK_GENES), axis=1).reshape(GENES)


def draw_genotypes(key, part):
    order_key = jax.random.fold_in(key, 11)
    shared_key = jax.random.fold_in(key, 12)
    own_key = jax.random.fold_in(key, 13)
    ranks = jax.random.permutation(order_key, BLOCKS).astype(jnp.float32)
    weights = 0.8 * ranks / max(BLOCKS - 1, 1)
    shared = jax.random.uniform(shared_key, (BLOCKS, 1, SAMPLES), dtype=jnp.float32, minval=0.0, maxval=2.0)
    own = jax.random.uniform(own_key, (BLOCKS, SPAN, SAMPLES), dtype=jnp.float32, minval=0.0, maxval=2.0)
    mixed = weights[:, None, None] * shared + (1.0 - weights[:, None, None]) * own
    return mixed.astype(jnp.bfloat16)


def steps_of(stream_key, dims, split, least, top_value):
    level, own = 1.0, jax.random.fold_in(stream_key, 6)
    for axis_at, shards_of in split:
        draws = jnp.exp(jax.random.uniform(jax.random.fold_in(own, axis_at), (shards_of,), jnp.float32, least / len(split), top_value / len(split)))
        level = level * jnp.repeat(draws, dims[axis_at] // shards_of).reshape([-1 if axis == axis_at else 1 for axis in range(len(dims))])
    return level


def bell_draw(key, dims, spread, limit, split=(), kind=jnp.bfloat16):
    values = spread * jax.random.normal(key, dims, jnp.float32)
    if split:
        values = values * steps_of(key, dims, split, -0.22, 0.18)
    return jnp.clip(values, -limit, limit).astype(kind)


def setup_inputs(seed: int = 0) -> dict:
    keys = jax.random.split(jax.random.key(seed), 5)
    return {
        "genotypes": draw_genotypes(jax.random.fold_in(keys[4], 71), 0),
        "phenotypes": bell_draw(keys[1], (GENES, SAMPLES), 1.0, 6.0, ((0, 8),), jnp.float32),
        "perm_rows": jax.vmap(lambda own: jax.random.permutation(own, SAMPLES))(jax.random.split(keys[2], PERMS)).reshape((PERMS, SAMPLES)).astype(jnp.int32),
        "starts": draw_starts(jax.random.fold_in(keys[4], 71), 0),
    }


def standard_rows(values):
    as_float = values.astype(jnp.float32)
    centred = as_float - lax.optimization_barrier(jnp.mean(as_float, axis=1, keepdims=True))
    inv_norm = lax.rsqrt(lax.optimization_barrier(jnp.sum(centred * centred, axis=1, keepdims=True)) + 1.0)
    return (centred * inv_norm).astype(jnp.bfloat16)

def reference(genotypes, phenotypes, perm_rows, starts):
    blocks = genotypes.shape[0]
    region = genotypes.shape[1]
    samples = phenotypes.shape[1]
    block_genes = phenotypes.shape[0] // blocks
    geno_std = jax.vmap(standard_rows)(genotypes)
    pheno_std = standard_rows(phenotypes).reshape(blocks, block_genes, samples)
    start_rows = starts.reshape(blocks, block_genes)
    positions = jnp.arange(region, dtype=jnp.int32)[None, :, None]
    in_window = (positions >= start_rows[:, None, :]) & (positions < start_rows[:, None, :] + WINDOW)
    perm_block = math.gcd(perm_rows.shape[0], 16)

    def per_perms(index_rows):

        def per_block(operands):
            rows_std, genes_std, window_mask = operands
            perm_table = jnp.take(genes_std.T, index_rows, axis=0)
            scores = jnp.einsum('vs,psg->vpg', rows_std.astype(jnp.float32), perm_table.astype(jnp.float32))
            return lax.optimization_barrier(jnp.max(jnp.where(window_mask[:, None, :], scores * scores, 0.0), axis=0))
        return lax.map(per_block, (geno_std, pheno_std, in_window))
    best_sq = lax.map(per_perms, perm_rows.reshape(-1, perm_block, samples))
    maxima = jnp.transpose(best_sq, (0, 2, 1, 3)).reshape(perm_rows.shape[0], blocks * block_genes) * samples
    log_stat = jnp.log1p(maxima)
    moments = jnp.stack((lax.optimization_barrier(jnp.sum(log_stat, axis=0)), lax.optimization_barrier(jnp.sum(log_stat * log_stat, axis=0)))) / perm_rows.shape[0]
    pooled = lax.optimization_barrier(jnp.sum(moments, axis=1)) / moments.shape[1]
    return (maxima, moments, pooled)
```

```python
import functools

import jax
import jax.numpy as jnp
from jax import lax
from jax.experimental import pallas as pl
from jax.experimental.pallas import tpu as pltpu
from jax.sharding import PartitionSpec as P

WINDOW = 4096
PERMS = 256
GROUP = 16
FOLD = 256
TILE = 256


def standardized(values):
    centred = values - jnp.mean(values, axis=1, keepdims=True)
    inv_norm = lax.rsqrt(jnp.sum(centred * centred, axis=1, keepdims=True) + 1.0)
    return (centred * inv_norm).astype(jnp.bfloat16)


def standard_kernel(x_ref, o_ref):
    o_ref[...] = standardized(x_ref[0].astype(jnp.float32))


def standard_rows(genotypes):
    _, rows, samples = genotypes.shape
    step = rows // 3
    return pl.pallas_call(
        standard_kernel,
        grid=(3,),
        in_specs=[pl.BlockSpec((1, step, samples), lambda i: (0, i, 0))],
        out_specs=pl.BlockSpec((step, samples), lambda i: (i, 0)),
        out_shape=jax.ShapeDtypeStruct((rows, samples), jnp.bfloat16),
        name="standard",
    )(genotypes)


def table_kernel(per_step, pheno_ref, perm_ref, out_ref, base_ref):
    genes, samples = pheno_ref.shape
    folds = samples // FOLD

    @pl.when(pl.program_id(0) == 0)
    def _():
        std = standardized(pheno_ref[...])
        for b in range(folds):
            base_ref[b * genes:(b + 1) * genes, :] = std[:, b * FOLD:(b + 1) * FOLD]

    within = lax.broadcasted_iota(jnp.int32, (FOLD, samples), 0)
    for k in range(per_step):
        index = perm_ref[0, k:k + 1, :]
        low = jnp.bitwise_and(index, FOLD - 1)
        block = jnp.right_shift(index, FOLD.bit_length() - 1)
        hot = jnp.where(within == low, 1.0, 0.0).astype(jnp.bfloat16)
        picked = jnp.dot(base_ref[...], hot, preferred_element_type=jnp.float32)
        chosen = picked[:genes]
        for b in range(1, folds):
            chosen = jnp.where(block == b, picked[b * genes:(b + 1) * genes], chosen)
        chosen = chosen.astype(jnp.bfloat16)
        for g in range(genes // GROUP):
            out_ref[g, k * GROUP:(k + 1) * GROUP, :] = chosen[g * GROUP:(g + 1) * GROUP]


def perm_tables(phenotypes, perm_rows):
    genes, samples = phenotypes.shape
    perms = perm_rows.shape[0]
    per_step = 4
    steps = perms // per_step
    return pl.pallas_call(
        functools.partial(table_kernel, per_step),
        grid=(steps,),
        in_specs=[
            pl.BlockSpec((genes, samples), lambda i: (0, 0)),
            pl.BlockSpec((1, per_step, samples), lambda i: (i, 0, 0)),
        ],
        out_specs=pl.BlockSpec((genes // GROUP, per_step * GROUP, samples), lambda i: (0, i, 0)),
        out_shape=jax.ShapeDtypeStruct((genes // GROUP, perms * GROUP, samples), jnp.bfloat16),
        scratch_shapes=[pltpu.VMEM((samples // FOLD * genes, FOLD), jnp.bfloat16)],
        name="tables",
    )(phenotypes, perm_rows.reshape(steps, per_step, samples))


def score_kernel(count, first_ref, table_ref, starts_ref, *refs):
    shards, out_ref, best_ref = refs[:count], refs[count], refs[count + 1]
    step = pl.program_id(0)
    rows = table_ref.shape[1]
    perms = rows // GROUP
    local = shards[0].shape[0]
    half = TILE // 2
    pieces = [(i, r) for i in range(count) for r in range(0, local, half)]
    lead = starts_ref[0]
    best = None
    for t in range(0, len(pieces), 2):
        pair = pieces[t:t + 2]
        weights = jnp.concatenate([shards[i][r:r + half, :] for i, r in pair], axis=0)
        scores = lax.dot_general(
            table_ref[0], weights, (((1,), (1,)), ((), ())), preferred_element_type=jnp.float32
        )
        for n, (i, r) in enumerate(pair):
            at = lax.broadcasted_iota(jnp.int32, (GROUP, half), 1) + (first_ref[i] + r)
            inside = (at >= lead) & (at < lead + WINDOW)
            part = jnp.abs(scores[:, n * half:(n + 1) * half]).reshape(perms, GROUP, half)
            part = jnp.where(inside[None], part, 0.0)
            best = part if best is None else jnp.maximum(best, part)
    best_ref[step] = best

    @pl.when(step == pl.num_programs(0) - 1)
    def _():
        groups = best_ref.shape[0]
        lane = lax.broadcasted_iota(jnp.int32, (1, GROUP, half), 2)
        gene = lax.broadcasted_iota(jnp.int32, (1, GROUP, half), 1)
        total = None
        for g in range(groups):
            top = jnp.max(best_ref[g], axis=2, keepdims=True)
            spread = jnp.max(jnp.where(lane == gene + g * GROUP, top, 0.0), axis=1)
            total = spread if total is None else jnp.maximum(total, spread)
        out_ref[...] = total


def window_best(table, starts, shards, firsts):
    groups, rows, samples = table.shape
    perms = rows // GROUP
    local = shards[0].shape[0]
    genes = groups * GROUP
    count = len(shards)
    lead = jnp.broadcast_to(starts.reshape(groups, GROUP, 1), (groups, GROUP, TILE // 2))
    whole = pl.BlockSpec((local, samples), lambda i: (0, 0), pipeline_mode=pl.Buffered(1))
    return pl.pallas_call(
        functools.partial(score_kernel, count),
        grid=(groups,),
        in_specs=[
            pl.BlockSpec(memory_space=pltpu.SMEM),
            pl.BlockSpec((1, rows, samples), lambda i: (i, 0, 0)),
            pl.BlockSpec((1, GROUP, TILE // 2), lambda i: (i, 0, 0)),
            *[whole] * count,
        ],
        out_specs=pl.BlockSpec((perms, genes), lambda i: (0, 0)),
        out_shape=jax.ShapeDtypeStruct((perms, genes), jnp.float32),
        scratch_shapes=[pltpu.VMEM((groups, perms, GROUP, TILE // 2), jnp.float32)],
        name="scores",
    )(jnp.stack(firsts).astype(jnp.int32), table, lead, *shards)


def shards_program(genotypes, phenotypes, perm_rows, starts):
    var_n = lax.axis_size("var")
    rows_n = var_n // 2
    both = ("var", "perm")
    samples = phenotypes.shape[1]
    local = genotypes.shape[1]
    gene_count = phenotypes.shape[0]

    def along(step):
        return [(v, ((v // 2 + step) % rows_n) * 2 + v % 2) for v in range(var_n)]

    twin = [(v, v ^ 1) for v in range(var_n)]
    across = [(0, 1), (1, 0)]
    mate = [
        (v * 2 + z, ((((v // 2 + rows_n // 2) % rows_n) * 2 + v % 2) * 2 + 1 - z))
        for v in range(var_n) for z in range(2)
    ]
    me = lax.axis_index("var")
    z = lax.axis_index("perm")
    y, core = me // 2, me % 2

    def first(row, c, deep):
        return ((((row + rows_n) % rows_n) * 2 + c) * 2 + deep) * local

    mate_rows = lax.ppermute(perm_rows, both, mate)
    own = standard_rows(genotypes)
    below = lax.ppermute(own, "var", along(1))
    above = lax.ppermute(own, "var", along(-1))
    deep = lax.ppermute(own, "perm", across)
    own_twin = lax.ppermute(own, "var", twin)
    table_own = perm_tables(phenotypes, perm_rows)
    table_mate = perm_tables(phenotypes, mate_rows)

    near = (own, own_twin)
    near_first = (first(y, core, z), first(y, 1 - core, z))
    far = [below, above, deep]
    far_at = [(y - 1, z), (y + 1, z), (y, 1 - z)]
    far_first = [first(a, core, d) for a, d in far_at] + [first(a, 1 - core, d) for a, d in far_at]
    far = far + [lax.ppermute(f, "var", twin) for f in far]

    near_own = window_best(table_own, starts, near, near_first)
    near_mate = window_best(table_mate, starts, near, near_first)
    far_mate = window_best(table_mate, starts, far, far_first)
    from_mate = lax.ppermute(jnp.maximum(near_mate, far_mate), both, mate)
    far_own = window_best(table_own, starts, far, far_first)
    best = jnp.maximum(jnp.maximum(near_own, far_own), from_mate)

    maxima = best * best * samples
    log_stat = jnp.log1p(maxima)
    sums = jnp.stack((jnp.sum(log_stat, axis=0), jnp.sum(log_stat * log_stat, axis=0)))
    everyone = ("gene", "var", "perm")
    count = lax.axis_size(everyone)
    blocks = lax.axis_size("gene")
    sent = lax.all_to_all(jnp.broadcast_to(sums[None], (count, *sums.shape)), everyone, 0, 0, tiled=True)
    per_block = jnp.sum(sent.reshape(blocks, count // blocks, *sums.shape), axis=1) / PERMS
    moments = lax.dynamic_index_in_dim(per_block, lax.axis_index("gene"), 0, keepdims=False)
    pooled = jnp.sum(per_block, axis=(0, 2)) / (gene_count * blocks)
    return (maxima, moments, pooled)


def solution(mesh):
    return jax.shard_map(
        shards_program,
        mesh=mesh,
        in_specs=(
            P("gene", ("var", "perm"), None),
            P("gene", None),
            P(("var", "perm"), None),
            P("gene"),
        ),
        out_specs=(P(("var", "perm"), "gene"), P(None, "gene"), P()),
        check_vma=False,
    )
```

```python
import functools

import jax
import jax.numpy as jnp
from jax import lax
from jax.experimental import pallas as pl
from jax.experimental.pallas import tpu as pltpu
from jax.sharding import PartitionSpec as P

WINDOW = 4096
PERMS = 256
FOLD = 256
TILE = 256
LARGE = 3.0e38


def standardized(values):
    centred = values - jnp.mean(values, axis=1, keepdims=True)
    inv_norm = lax.rsqrt(jnp.sum(centred * centred, axis=1, keepdims=True) + 1.0)
    return (centred * inv_norm).astype(jnp.bfloat16)


def standard_kernel(x_ref, o_ref):
    o_ref[...] = standardized(x_ref[0].astype(jnp.float32))


def standard_rows(genotypes):
    _, rows, samples = genotypes.shape
    step = rows // 3
    return pl.pallas_call(
        standard_kernel,
        grid=(3,),
        in_specs=[pl.BlockSpec((1, step, samples), lambda i: (0, i, 0))],
        out_specs=pl.BlockSpec((step, samples), lambda i: (i, 0)),
        out_shape=jax.ShapeDtypeStruct((rows, samples), jnp.bfloat16),
        cost_estimate=cost(8 * rows * samples),
        compiler_params=params(16),
        name="standard",
    )(genotypes)


def cost(flops):
    return pl.CostEstimate(flops=flops, bytes_accessed=0, transcendentals=0)


def places(local):
    var_n, me, z = lax.axis_size("var"), lax.axis_index("var"), lax.axis_index("perm")
    rows_n = var_n // 2
    y, core = lax.div(me, 2), lax.rem(me, 2)

    def first(up, same_core, same_depth):
        c = core if same_core else 1 - core
        d = z if same_depth else 1 - z
        return ((lax.rem(y + up + rows_n, rows_n) * 2 + c) * 2 + d) * local

    near = [first(0, True, True), first(0, False, True)]
    far = [first(u, c, d) for c in (True, False) for u, d in ((-1, True), (1, True), (0, False))]
    return near, far


def fill_masks(firsts, lead, mask_ref, local):
    half = TILE // 2
    lane = lax.broadcasted_iota(jnp.int32, lead.shape, 1)
    for i in range(len(firsts)):
        for r in range(0, local, half):
            past = lane + (firsts[i] + r) - lead
            inside = (past >= 0) & (past < WINDOW)
            at = i * local + r
            mask_ref[:, at:at + half] = jnp.where(inside, LARGE, 0.0)


def weight_tiles(shards, local):
    half = TILE // 2
    pieces = [(i, r) for i in range(len(shards)) for r in range(0, local, half)]
    for t in range(0, len(pieces), 2):
        pair = pieces[t:t + 2]
        yield t * half, jnp.concatenate([shards[i][r:r + half, :] for i, r in pair], axis=0)


def lane_best(rows_bf16, shards, local, mask_ref, copies):
    half = TILE // 2
    genes = mask_ref.shape[0]
    best = None
    for at, weights in weight_tiles(shards, local):
        scores = lax.dot_general(
            rows_bf16, weights, (((1,), (1,)), ((), ())), preferred_element_type=jnp.float32
        )
        for n in range(weights.shape[0] // half):
            part = jnp.abs(scores[:, n * half:(n + 1) * half]).reshape(copies, genes, half)
            part = jnp.minimum(part, mask_ref[:, at + n * half:at + (n + 1) * half][None])
            best = part if best is None else jnp.maximum(best, part)
    return best


def reduce_lanes(best_ref, out_ref):
    perms, genes, half = best_ref.shape
    lane = lax.broadcasted_iota(jnp.int32, (genes, half), 1)
    gene = lax.broadcasted_iota(jnp.int32, (genes, half), 0)
    for p in range(perms):
        top = jnp.max(best_ref[p], axis=1, keepdims=True)
        out_ref[p:p + 1, :] = jnp.max(jnp.where(lane == gene, top, 0.0), axis=0, keepdims=True)


def near_kernel(per_step, pheno_ref, perm_ref, mate_ref, starts_ref, own_ref, twin_ref,
                table_ref, out_ref, lead_ref, base_ref, rows_ref, mask_ref, best_ref):
    genes, samples = pheno_ref.shape
    folds = samples // FOLD
    local = own_ref.shape[0]
    half_perms = perm_ref.shape[0]
    step = pl.program_id(0)

    @pl.when(step == 0)
    def _():
        std = standardized(pheno_ref[...])
        for b in range(folds):
            base_ref[b * genes:(b + 1) * genes, :] = std[:, b * FOLD:(b + 1) * FOLD]
        rows_ref[:half_perms, :] = perm_ref[...]
        rows_ref[half_perms:, :] = mate_ref[...]
        wide = jnp.broadcast_to(starts_ref[...].astype(jnp.float32), lead_ref.shape)
        lead = wide.T.astype(jnp.int32)
        lead_ref[...] = lead
        fill_masks(places(local)[0], lead, mask_ref, local)

    within = lax.broadcasted_iota(jnp.int32, (FOLD, samples), 0)
    for k in range(per_step):
        index = rows_ref[pl.ds(step * per_step + k, 1), :]
        low = jnp.bitwise_and(index, FOLD - 1)
        block = jnp.right_shift(index, FOLD.bit_length() - 1)
        hot = jnp.where(within == low, 1.0, 0.0).astype(jnp.bfloat16)
        picked = jnp.dot(base_ref[...], hot, preferred_element_type=jnp.float32)
        chosen = picked[:genes]
        for b in range(1, folds):
            chosen = jnp.where(block == b, picked[b * genes:(b + 1) * genes], chosen)
        table_ref[k * genes:(k + 1) * genes, :] = chosen.astype(jnp.bfloat16)
    best = lane_best(table_ref[...], (own_ref, twin_ref), local, mask_ref, per_step)
    best_ref[pl.ds(step * per_step, per_step)] = best

    @pl.when(step == pl.num_programs(0) - 1)
    def _():
        reduce_lanes(best_ref, out_ref)


def params(limit):
    return pltpu.CompilerParams(vmem_limit_bytes=limit * 1024 * 1024)


def near_best(phenotypes, perm_rows, mate_rows, starts, shards):
    genes, samples = phenotypes.shape
    perms = perm_rows.shape[0] + mate_rows.shape[0]
    local = shards[0].shape[0]
    per_step = 2
    once = pl.Buffered(1)

    def whole(shape):
        return pl.BlockSpec(shape, lambda i: (0, 0), pipeline_mode=once)

    return pl.pallas_call(
        functools.partial(near_kernel, per_step),
        grid=(perms // per_step,),
        in_specs=[
            whole((genes, samples)),
            whole(perm_rows.shape),
            whole(mate_rows.shape),
            whole((1, genes)),
            whole((local, samples)),
            whole((local, samples)),
        ],
        out_specs=[
            pl.BlockSpec((per_step * genes, samples), lambda i: (i, 0)),
            pl.BlockSpec((perms, genes), lambda i: (0, 0)),
            pl.BlockSpec((genes, TILE // 2), lambda i: (0, 0)),
        ],
        out_shape=[
            jax.ShapeDtypeStruct((perms * genes, samples), jnp.bfloat16),
            jax.ShapeDtypeStruct((perms, genes), jnp.float32),
            jax.ShapeDtypeStruct((genes, TILE // 2), jnp.int32),
        ],
        scratch_shapes=[
            pltpu.VMEM((samples // FOLD * genes, FOLD), jnp.bfloat16),
            pltpu.VMEM((perms, samples), jnp.int32),
            pltpu.VMEM((genes, 2 * local), jnp.float32),
            pltpu.VMEM((perms, genes, TILE // 2), jnp.float32),
        ],
        cost_estimate=cost(2 * perms * genes * samples * (2 * local + samples)),
        compiler_params=params(24),
        name="near",
    )(phenotypes, perm_rows, mate_rows, starts.reshape(1, genes), *shards)


def far_kernel(count, per_step, table_ref, lead_ref, before_ref, *refs):
    shards, (out_ref, mask_ref, best_ref) = refs[:count], refs[count:]
    local = shards[0].shape[0]
    step = pl.program_id(0)

    @pl.when(step == 0)
    def _():
        fill_masks(places(local)[1], lead_ref[...], mask_ref, local)

    best = lane_best(table_ref[...], shards, local, mask_ref, per_step)
    best_ref[pl.ds(step * per_step, per_step)] = best

    @pl.when(step == pl.num_programs(0) - 1)
    def _():
        reduce_lanes(best_ref, out_ref)
        out_ref[...] = jnp.maximum(out_ref[...], before_ref[...])


def far_best(table, part, lead, before, shards):
    samples = table.shape[1]
    genes = lead.shape[0]
    perms = before.shape[0] // 2
    local = shards[0].shape[0]
    count = len(shards)
    per_step = 2
    steps = perms // per_step
    once = pl.Buffered(1)
    whole = pl.BlockSpec((local, samples), lambda i: (0, 0), pipeline_mode=once)
    return pl.pallas_call(
        functools.partial(far_kernel, count, per_step),
        grid=(steps,),
        in_specs=[
            pl.BlockSpec((per_step * genes, samples), lambda i: (i + part * steps, 0)),
            pl.BlockSpec(lead.shape, lambda i: (0, 0), pipeline_mode=once),
            pl.BlockSpec((perms, genes), lambda i: (part, 0), pipeline_mode=once),
            *[whole] * count,
        ],
        out_specs=pl.BlockSpec((perms, genes), lambda i: (0, 0)),
        out_shape=jax.ShapeDtypeStruct((perms, genes), jnp.float32),
        scratch_shapes=[
            pltpu.VMEM((genes, count * local), jnp.float32),
            pltpu.VMEM((perms, genes, TILE // 2), jnp.float32),
        ],
        cost_estimate=cost(2 * perms * genes * samples * count * local),
        compiler_params=params(24),
        name="far",
    )(table, lead, before, *shards)


def finish_kernel(spread, best_ref, mate_ref, maxima_ref, sums_ref, *, samples):
    best = jnp.maximum(best_ref[...], mate_ref[...])
    maxima = best * best * samples
    maxima_ref[...] = maxima
    log_stat = jnp.log1p(maxima)
    sums = jnp.stack((jnp.sum(log_stat, axis=0), jnp.sum(log_stat * log_stat, axis=0)))
    sums_ref[...] = jnp.broadcast_to(sums[None], sums_ref.shape)


def finished(best, from_mate, samples, spread):
    perms, genes = best.shape
    return pl.pallas_call(
        functools.partial(finish_kernel, spread, samples=samples),
        out_shape=[
            jax.ShapeDtypeStruct((perms, genes), jnp.float32),
            jax.ShapeDtypeStruct((spread, 2, genes), jnp.float32),
        ],
        compiler_params=params(4),
        name="finish",
    )(best, from_mate)


def shards_program(genotypes, phenotypes, perm_rows, starts):
    var_n = lax.axis_size("var")
    rows_n = var_n // 2
    both = ("var", "perm")
    samples = phenotypes.shape[1]
    gene_count = phenotypes.shape[0]

    def along(step):
        return [(v, ((v // 2 + step) % rows_n) * 2 + v % 2) for v in range(var_n)]

    twin = [(v, v ^ 1) for v in range(var_n)]
    across = [(0, 1), (1, 0)]
    mate = [
        (v * 2 + z, ((((v // 2 + rows_n // 2) % rows_n) * 2 + v % 2) * 2 + 1 - z))
        for v in range(var_n) for z in range(2)
    ]

    mate_rows = lax.ppermute(perm_rows, both, mate)
    own = standard_rows(genotypes)
    below = lax.ppermute(own, "var", along(1))
    above = lax.ppermute(own, "var", along(-1))
    deep = lax.ppermute(own, "perm", across)
    own_twin = lax.ppermute(own, "var", twin)
    table, near, lead = near_best(phenotypes, perm_rows, mate_rows, starts, (own, own_twin))
    below, above, deep, lead = lax.optimization_barrier((below, above, deep, lead))
    far = [below, above, deep]
    far = far + [lax.ppermute(f, "var", twin) for f in far]
    to_mate = far_best(table, 1, lead, near, far)
    from_mate = lax.ppermute(to_mate, both, mate)
    best = far_best(table, 0, lead, near, far)
    count = lax.axis_size(("gene", "var", "perm"))
    maxima, sums = finished(best, from_mate, samples, count)

    everyone = ("gene", "var", "perm")
    blocks = lax.axis_size("gene")
    sent = lax.all_to_all(sums, everyone, 0, 0, tiled=True)
    per_block = jnp.sum(sent.reshape(blocks, count // blocks, *sums.shape[1:]), axis=1) / PERMS
    moments = lax.dynamic_index_in_dim(per_block, lax.axis_index("gene"), 0, keepdims=False)
    pooled = jnp.sum(per_block, axis=(0, 2)) / (gene_count * blocks)
    return (maxima, moments, pooled)


def solution(mesh):
    return jax.shard_map(
        shards_program,
        mesh=mesh,
        in_specs=(
            P("gene", ("var", "perm"), None),
            P("gene", None),
            P(("var", "perm"), None),
            P("gene"),
        ),
        out_specs=(P(("var", "perm"), "gene"), P(None, "gene"), P()),
        check_vma=False,
    )
```

```python
import functools

import jax
import jax.numpy as jnp
from jax import lax
from jax.experimental import pallas as pl
from jax.experimental.pallas import tpu as pltpu
from jax.sharding import PartitionSpec as P

WINDOW = 4096
PERMS = 256
FOLD = 256
TILE = 256
LARGE = 3.0e38


def standardized(values):
    centred = values - jnp.mean(values, axis=1, keepdims=True)
    inv_norm = lax.rsqrt(jnp.sum(centred * centred, axis=1, keepdims=True) + 1.0)
    return (centred * inv_norm).astype(jnp.bfloat16)


def standard_kernel(x_ref, o_ref):
    o_ref[...] = standardized(x_ref[0].astype(jnp.float32))


def standard_rows(genotypes):
    _, rows, samples = genotypes.shape
    step = rows // 3
    return pl.pallas_call(
        standard_kernel,
        grid=(3,),
        in_specs=[pl.BlockSpec((1, step, samples), lambda i: (0, i, 0))],
        out_specs=pl.BlockSpec((step, samples), lambda i: (i, 0)),
        out_shape=jax.ShapeDtypeStruct((rows, samples), jnp.bfloat16),
        cost_estimate=cost(8 * rows * samples),
        compiler_params=params(16),
        name="standard",
    )(genotypes)


def cost(flops):
    return pl.CostEstimate(flops=flops, bytes_accessed=0, transcendentals=0)


def places(local):
    var_n, me, z = lax.axis_size("var"), lax.axis_index("var"), lax.axis_index("perm")
    rows_n = var_n // 2
    y, core = lax.div(me, 2), lax.rem(me, 2)

    def first(up, same_core, same_depth):
        c = core if same_core else 1 - core
        d = z if same_depth else 1 - z
        return ((lax.rem(y + up + rows_n, rows_n) * 2 + c) * 2 + d) * local

    near = [first(0, True, True), first(0, False, True)]
    far = [first(u, c, d) for c in (True, False) for u, d in ((-1, True), (1, True), (0, False))]
    return near, far


def fill_masks(firsts, lead, mask_ref, local):
    half = TILE // 2
    lane = lax.broadcasted_iota(jnp.int32, lead.shape, 1)
    for i in range(len(firsts)):
        for r in range(0, local, half):
            past = lane + (firsts[i] + r) - lead
            inside = (past >= 0) & (past < WINDOW)
            at = i * local + r
            mask_ref[:, at:at + half] = jnp.where(inside, LARGE, 0.0)


def weight_tiles(shards, local):
    half = TILE // 2
    pieces = [(i, r) for i in range(len(shards)) for r in range(0, local, half)]
    for t in range(0, len(pieces), 2):
        pair = pieces[t:t + 2]
        yield t * half, jnp.concatenate([shards[i][r:r + half, :] for i, r in pair], axis=0)


def lane_best(rows_bf16, shards, local, mask_ref, copies):
    half = TILE // 2
    genes = mask_ref.shape[0]
    best = None
    for at, weights in weight_tiles(shards, local):
        scores = lax.dot_general(
            rows_bf16, weights, (((1,), (1,)), ((), ())), preferred_element_type=jnp.float32
        )
        for n in range(weights.shape[0] // half):
            part = jnp.abs(scores[:, n * half:(n + 1) * half]).reshape(copies, genes, half)
            part = jnp.minimum(part, mask_ref[:, at + n * half:at + (n + 1) * half][None])
            best = part if best is None else jnp.maximum(best, part)
    return best


def reduce_lanes(best_ref, out_ref):
    perms, genes, half = best_ref.shape
    lane = lax.broadcasted_iota(jnp.int32, (genes, half), 1)
    gene = lax.broadcasted_iota(jnp.int32, (genes, half), 0)
    for p in range(perms):
        top = jnp.max(best_ref[p], axis=1, keepdims=True)
        out_ref[p:p + 1, :] = jnp.max(jnp.where(lane == gene, top, 0.0), axis=0, keepdims=True)


def near_kernel(per_step, pheno_ref, perm_ref, mate_ref, starts_ref, own_ref, twin_ref,
                table_ref, out_ref, lead_ref, base_ref, rows_ref, mask_ref, best_ref):
    genes, samples = pheno_ref.shape
    folds = samples // FOLD
    local = own_ref.shape[0]
    half_perms = perm_ref.shape[0]
    step = pl.program_id(0)

    @pl.when(step == 0)
    def _():
        std = standardized(pheno_ref[...])
        for b in range(folds):
            base_ref[b * genes:(b + 1) * genes, :] = std[:, b * FOLD:(b + 1) * FOLD]
        rows_ref[:half_perms, :] = perm_ref[...]
        rows_ref[half_perms:, :] = mate_ref[...]
        wide = jnp.broadcast_to(starts_ref[...].astype(jnp.float32), lead_ref.shape)
        lead = wide.T.astype(jnp.int32)
        lead_ref[...] = lead
        fill_masks(places(local)[0], lead, mask_ref, local)

    within = lax.broadcasted_iota(jnp.int32, (FOLD, samples), 0)
    for k in range(per_step):
        index = rows_ref[pl.ds(step * per_step + k, 1), :]
        low = jnp.bitwise_and(index, FOLD - 1)
        block = jnp.right_shift(index, FOLD.bit_length() - 1)
        hot = jnp.where(within == low, 1.0, 0.0).astype(jnp.bfloat16)
        picked = jnp.dot(base_ref[...], hot, preferred_element_type=jnp.float32)
        chosen = picked[:genes]
        for b in range(1, folds):
            chosen = jnp.where(block == b, picked[b * genes:(b + 1) * genes], chosen)
        table_ref[k * genes:(k + 1) * genes, :] = chosen.astype(jnp.bfloat16)
    best = lane_best(table_ref[...], (own_ref, twin_ref), local, mask_ref, per_step)
    best_ref[pl.ds(step * per_step, per_step)] = best

    @pl.when(step == pl.num_programs(0) - 1)
    def _():
        reduce_lanes(best_ref, out_ref)


def params(limit):
    return pltpu.CompilerParams(vmem_limit_bytes=limit * 1024 * 1024)


def in_hbm(array):
    return pltpu.with_memory_space_constraint(array, pltpu.HBM)


def near_best(phenotypes, perm_rows, mate_rows, starts, shards):
    genes, samples = phenotypes.shape
    perms = perm_rows.shape[0] + mate_rows.shape[0]
    local = shards[0].shape[0]
    per_step = 4
    once = pl.Buffered(1)

    def whole(shape):
        return pl.BlockSpec(shape, lambda i: (0, 0), pipeline_mode=once)

    return pl.pallas_call(
        functools.partial(near_kernel, per_step),
        grid=(perms // per_step,),
        in_specs=[
            whole((genes, samples)),
            whole(perm_rows.shape),
            whole(mate_rows.shape),
            whole((1, genes)),
            whole((local, samples)),
            whole((local, samples)),
        ],
        out_specs=[
            pl.BlockSpec((per_step * genes, samples), lambda i: (i, 0)),
            pl.BlockSpec((perms, genes), lambda i: (0, 0)),
            pl.BlockSpec((genes, TILE // 2), lambda i: (0, 0)),
        ],
        out_shape=[
            jax.ShapeDtypeStruct((perms * genes, samples), jnp.bfloat16),
            jax.ShapeDtypeStruct((perms, genes), jnp.float32),
            jax.ShapeDtypeStruct((genes, TILE // 2), jnp.int32),
        ],
        scratch_shapes=[
            pltpu.VMEM((samples // FOLD * genes, FOLD), jnp.bfloat16),
            pltpu.VMEM((perms, samples), jnp.int32),
            pltpu.VMEM((genes, 2 * local), jnp.float32),
            pltpu.VMEM((perms, genes, TILE // 2), jnp.float32),
        ],
        cost_estimate=cost(2 * perms * genes * samples * (2 * local + samples)),
        compiler_params=params(24),
        name="near",
    )(in_hbm(phenotypes), in_hbm(perm_rows), mate_rows, in_hbm(starts.reshape(1, genes)), *shards)


def far_kernel(count, per_step, table_ref, lead_ref, before_ref, *refs):
    shards, (out_ref, mask_ref, best_ref) = refs[:count], refs[count:]
    local = shards[0].shape[0]
    step = pl.program_id(0)

    @pl.when(step == 0)
    def _():
        fill_masks(places(local)[1], lead_ref[...], mask_ref, local)

    best = lane_best(table_ref[...], shards, local, mask_ref, per_step)
    best_ref[pl.ds(step * per_step, per_step)] = best

    @pl.when(step == pl.num_programs(0) - 1)
    def _():
        reduce_lanes(best_ref, out_ref)
        out_ref[...] = jnp.maximum(out_ref[...], before_ref[...])


def far_best(table, part, lead, before, shards):
    samples = table.shape[1]
    genes = lead.shape[0]
    perms = before.shape[0] // 2
    local = shards[0].shape[0]
    count = len(shards)
    per_step = 8
    steps = perms // per_step
    once = pl.Buffered(1)
    whole = pl.BlockSpec((local, samples), lambda i: (0, 0), pipeline_mode=once)
    return pl.pallas_call(
        functools.partial(far_kernel, count, per_step),
        grid=(steps,),
        in_specs=[
            pl.BlockSpec((per_step * genes, samples), lambda i: (i + part * steps, 0)),
            pl.BlockSpec(lead.shape, lambda i: (0, 0), pipeline_mode=once),
            pl.BlockSpec((perms, genes), lambda i: (part, 0), pipeline_mode=once),
            *[whole] * count,
        ],
        out_specs=pl.BlockSpec((perms, genes), lambda i: (0, 0)),
        out_shape=jax.ShapeDtypeStruct((perms, genes), jnp.float32),
        scratch_shapes=[
            pltpu.VMEM((genes, count * local), jnp.float32),
            pltpu.VMEM((perms, genes, TILE // 2), jnp.float32),
        ],
        cost_estimate=cost(2 * perms * genes * samples * count * local),
        compiler_params=params(24),
        name="far",
    )(table, lead, before, *shards)


def finish_kernel(spread, best_ref, mate_ref, maxima_ref, sums_ref, *, samples):
    best = jnp.maximum(best_ref[...], mate_ref[...])
    maxima = best * best * samples
    maxima_ref[...] = maxima
    log_stat = jnp.log1p(maxima)
    sums = jnp.stack((jnp.sum(log_stat, axis=0), jnp.sum(log_stat * log_stat, axis=0)))
    sums_ref[...] = jnp.broadcast_to(sums[None], sums_ref.shape)


def finished(best, from_mate, samples, spread):
    perms, genes = best.shape
    return pl.pallas_call(
        functools.partial(finish_kernel, spread, samples=samples),
        out_shape=[
            jax.ShapeDtypeStruct((perms, genes), jnp.float32),
            jax.ShapeDtypeStruct((spread, 2, genes), jnp.float32),
        ],
        compiler_params=params(4),
        name="finish",
    )(best, from_mate)


def totals_kernel(sent_ref, moments_ref, pooled_ref):
    count, _, genes = sent_ref.shape
    blocks = lax.axis_size("gene")
    members = count // blocks
    mine = pl.multiple_of(lax.axis_index("gene") * members, members)
    moments_ref[...] = jnp.sum(sent_ref[pl.ds(mine, members)], axis=0) / PERMS
    every = jnp.sum(sent_ref[...], axis=0) / PERMS
    both = jnp.sum(every, axis=1, keepdims=True) / (genes * blocks)
    lane = lax.broadcasted_iota(jnp.int32, every.shape, 1)
    row = lax.broadcasted_iota(jnp.int32, every.shape, 0)
    spread = jnp.sum(jnp.where(lane == row, both, 0.0), axis=0, keepdims=True)
    pooled_ref[...] = spread[:, :2]


def totals(sent):
    return pl.pallas_call(
        totals_kernel,
        out_shape=[
            jax.ShapeDtypeStruct(sent.shape[1:], jnp.float32),
            jax.ShapeDtypeStruct((1, 2), jnp.float32),
        ],
        compiler_params=params(4),
        name="totals",
    )(sent)


def shards_program(genotypes, phenotypes, perm_rows, starts):
    var_n = lax.axis_size("var")
    rows_n = var_n // 2
    both = ("var", "perm")
    samples = phenotypes.shape[1]

    def along(step):
        return [(v, ((v // 2 + step) % rows_n) * 2 + v % 2) for v in range(var_n)]

    twin = [(v, v ^ 1) for v in range(var_n)]
    across = [(0, 1), (1, 0)]
    mate = [
        (v * 2 + z, ((((v // 2 + rows_n // 2) % rows_n) * 2 + v % 2) * 2 + 1 - z))
        for v in range(var_n) for z in range(2)
    ]

    mate_rows = lax.ppermute(perm_rows, both, mate)
    own = standard_rows(genotypes)
    below = lax.ppermute(own, "var", along(1))
    above = lax.ppermute(own, "var", along(-1))
    deep = lax.ppermute(own, "perm", across)
    own_twin = lax.ppermute(own, "var", twin)
    table, near, lead = near_best(phenotypes, perm_rows, mate_rows, starts, (own, own_twin))
    below, above, deep, lead = lax.optimization_barrier((below, above, deep, lead))
    far = [below, above, deep]
    far = far + [lax.ppermute(f, "var", twin) for f in far]
    to_mate = far_best(table, 1, lead, near, far)
    from_mate = lax.ppermute(to_mate, both, mate)
    best = far_best(table, 0, lead, near, far)
    count = lax.axis_size(("gene", "var", "perm"))
    maxima, sums = finished(best, from_mate, samples, count)

    sent = lax.all_to_all(sums, ("gene", "var", "perm"), 0, 0, tiled=True)
    moments, pooled = totals(sent)
    return (maxima, moments, pooled.reshape(2))


def solution(mesh):
    return jax.shard_map(
        shards_program,
        mesh=mesh,
        in_specs=(
            P("gene", ("var", "perm"), None),
            P("gene", None),
            P(("var", "perm"), None),
            P("gene"),
        ),
        out_specs=(P(("var", "perm"), "gene"), P(None, "gene"), P()),
        check_vma=False,
    )
```

```python
import functools

import jax
import jax.numpy as jnp
from jax import lax
from jax.experimental import pallas as pl
from jax.experimental.pallas import tpu as pltpu
from jax.sharding import PartitionSpec as P

WINDOW = 4096
PERMS = 256
FOLD = 256
TILE = 256
LARGE = 3.0e38


def standardized(values):
    centred = values - jnp.mean(values, axis=1, keepdims=True)
    inv_norm = lax.rsqrt(jnp.sum(centred * centred, axis=1, keepdims=True) + 1.0)
    return (centred * inv_norm).astype(jnp.bfloat16)


def standard_kernel(x_ref, o_ref):
    o_ref[...] = standardized(x_ref[0].astype(jnp.float32))


def standard_rows(genotypes):
    _, rows, samples = genotypes.shape
    step = rows // 3
    return pl.pallas_call(
        standard_kernel,
        grid=(3,),
        in_specs=[pl.BlockSpec((1, step, samples), lambda i: (0, i, 0))],
        out_specs=pl.BlockSpec((step, samples), lambda i: (i, 0)),
        out_shape=jax.ShapeDtypeStruct((rows, samples), jnp.bfloat16),
        cost_estimate=cost(8 * rows * samples),
        compiler_params=params(16),
        name="standard",
    )(genotypes)


def cost(flops):
    return pl.CostEstimate(flops=flops, bytes_accessed=0, transcendentals=0)


def places(local):
    var_n, me, z = lax.axis_size("var"), lax.axis_index("var"), lax.axis_index("perm")
    rows_n = var_n // 2
    y, core = lax.div(me, 2), lax.rem(me, 2)

    def first(up, same_core, same_depth):
        c = core if same_core else 1 - core
        d = z if same_depth else 1 - z
        return ((lax.rem(y + up + rows_n, rows_n) * 2 + c) * 2 + d) * local

    near = [first(0, True, True), first(0, False, True)]
    far = [first(u, c, d) for c in (True, False) for u, d in ((-1, True), (1, True), (0, False))]
    return near, far


def window_mask(first, lead, width):
    half = TILE // 2
    lane = lax.broadcasted_iota(jnp.int32, lead.shape, 1)
    masks = []
    for r in range(0, width, half):
        past = lane + (first + r) - lead
        masks.append(jnp.where((past >= 0) & (past < WINDOW), LARGE, 0.0))
    return jnp.concatenate(masks, axis=1)


def weight_tiles(shards, local):
    half = TILE // 2
    pieces = [(i, r) for i in range(len(shards)) for r in range(0, local, half)]
    for t in range(0, len(pieces), 2):
        pair = pieces[t:t + 2]
        yield t * half, jnp.concatenate([shards[i][r:r + half, :] for i, r in pair], axis=0)


def lane_best(rows_bf16, shards, local, masks, copies):
    half = TILE // 2
    best = None
    for at, weights in weight_tiles(shards, local):
        scores = lax.dot_general(
            rows_bf16, weights, (((1,), (1,)), ((), ())), preferred_element_type=jnp.float32
        )
        for n in range(weights.shape[0] // half):
            i, r = divmod(at + n * half, local)
            mask_ref, k = masks[i]
            mask = mask_ref[k, :, r:r + half]
            part = jnp.abs(scores[:, n * half:(n + 1) * half]).reshape(copies, mask.shape[0], half)
            part = jnp.minimum(part, mask[None])
            best = part if best is None else jnp.maximum(best, part)
    return best


def reduce_lanes(best_ref, slot, out_ref, row):
    _, perms, genes, half = best_ref.shape
    lane = lax.broadcasted_iota(jnp.int32, (genes, half), 1)
    gene = lax.broadcasted_iota(jnp.int32, (genes, half), 0)
    for p in range(perms):
        top = jnp.max(best_ref[slot, p], axis=1, keepdims=True)
        best = jnp.max(jnp.where(lane == gene, top, 0.0), axis=0, keepdims=True)
        out_ref[pl.ds(row + p, 1), :] = best


def score_step(rows_bf16, shards, local, masks, per_step, best_ref, out_ref):
    step = pl.program_id(0)
    slot = lax.rem(step, 2)
    reduce_lanes(best_ref, 1 - slot, out_ref, jnp.maximum(step - 1, 0) * per_step)
    best_ref[slot] = lane_best(rows_bf16, shards, local, masks, per_step)

    @pl.when(step == pl.num_programs(0) - 1)
    def _():
        reduce_lanes(best_ref, slot, out_ref, step * per_step)


def near_kernel(per_step, pheno_ref, perm_ref, mate_ref, starts_ref, own_ref, twin_ref,
                table_ref, out_ref, far_mask_ref, base_ref, rows_ref, lead_ref, mask_ref, best_ref):
    genes, samples = pheno_ref.shape
    folds = samples // FOLD
    local = own_ref.shape[0]
    half_perms = perm_ref.shape[0]
    step = pl.program_id(0)
    near_first, far_first = places(local)

    @pl.when(step == 0)
    def _():
        std = standardized(pheno_ref[...])
        for b in range(folds):
            base_ref[b * genes:(b + 1) * genes, :] = std[:, b * FOLD:(b + 1) * FOLD]
        rows_ref[:half_perms, :] = perm_ref[...]
        rows_ref[half_perms:, :] = mate_ref[...]
        wide = jnp.broadcast_to(starts_ref[...].astype(jnp.float32), lead_ref.shape)
        lead = wide.T.astype(jnp.int32)
        lead_ref[...] = lead
        for i in range(2):
            mask_ref[i] = window_mask(near_first[i], lead, local)

    shard = jnp.minimum(step, len(far_first) - 1)
    first = far_first[0]
    for i in range(1, len(far_first)):
        first = jnp.where(shard == i, far_first[i], first)
    far_mask_ref[shard] = window_mask(first, lead_ref[...], local)

    within = lax.broadcasted_iota(jnp.int32, (FOLD, samples), 0)
    for k in range(per_step):
        index = rows_ref[pl.ds(step * per_step + k, 1), :]
        low = jnp.bitwise_and(index, FOLD - 1)
        block = jnp.right_shift(index, FOLD.bit_length() - 1)
        hot = jnp.where(within == low, 1.0, 0.0).astype(jnp.bfloat16)
        picked = jnp.dot(base_ref[...], hot, preferred_element_type=jnp.float32)
        chosen = picked[:genes]
        for b in range(1, folds):
            chosen = jnp.where(block == b, picked[b * genes:(b + 1) * genes], chosen)
        table_ref[k * genes:(k + 1) * genes, :] = chosen.astype(jnp.bfloat16)
    masks = [(mask_ref, 0), (mask_ref, 1)]
    score_step(table_ref[...], (own_ref, twin_ref), local, masks, per_step, best_ref, out_ref)


def params(limit):
    return pltpu.CompilerParams(vmem_limit_bytes=limit * 1024 * 1024)


def in_hbm(array):
    return pltpu.with_memory_space_constraint(array, pltpu.HBM)


def near_best(phenotypes, perm_rows, mate_rows, starts, shards):
    genes, samples = phenotypes.shape
    perms = perm_rows.shape[0] + mate_rows.shape[0]
    local = shards[0].shape[0]
    per_step = 4
    once = pl.Buffered(1)

    def whole(shape):
        return pl.BlockSpec(shape, lambda i: (0, 0), pipeline_mode=once)

    return pl.pallas_call(
        functools.partial(near_kernel, per_step),
        grid=(perms // per_step,),
        in_specs=[
            whole((genes, samples)),
            whole(perm_rows.shape),
            whole(mate_rows.shape),
            whole((1, genes)),
            whole((local, samples)),
            whole((local, samples)),
        ],
        out_specs=[
            pl.BlockSpec((per_step * genes, samples), lambda i: (i, 0)),
            pl.BlockSpec((perms, genes), lambda i: (0, 0)),
            pl.BlockSpec((6, genes, local), lambda i: (0, 0, 0)),
        ],
        out_shape=[
            jax.ShapeDtypeStruct((perms * genes, samples), jnp.bfloat16),
            jax.ShapeDtypeStruct((perms, genes), jnp.float32),
            jax.ShapeDtypeStruct((6, genes, local), jnp.float32),
        ],
        scratch_shapes=[
            pltpu.VMEM((samples // FOLD * genes, FOLD), jnp.bfloat16),
            pltpu.VMEM((perms, samples), jnp.int32),
            pltpu.VMEM((genes, TILE // 2), jnp.int32),
            pltpu.VMEM((2, genes, local), jnp.float32),
            pltpu.VMEM((2, per_step, genes, TILE // 2), jnp.float32),
        ],
        cost_estimate=cost(2 * perms * genes * samples * (2 * local + samples)),
        compiler_params=params(24),
        name="near",
    )(in_hbm(phenotypes), in_hbm(perm_rows), mate_rows, in_hbm(starts.reshape(1, genes)), *shards)


def far_kernel(pairs, per_step, table_ref, before_ref, *refs):
    count = 2 * pairs
    shards, mask_refs, (out_ref, best_ref) = refs[:count], refs[count:count + pairs], refs[count + pairs:]
    local = shards[0].shape[0]
    masks = [(m, k) for m in mask_refs for k in range(2)]
    score_step(table_ref[...], shards, local, masks, per_step, best_ref, out_ref)

    @pl.when(pl.program_id(0) == pl.num_programs(0) - 1)
    def _():
        out_ref[...] = jnp.maximum(out_ref[...], before_ref[...])


def far_best(table, part, before, before_part, masks, pairs, shards):
    samples = table.shape[1]
    _, genes, local = masks.shape
    perms = table.shape[0] // genes // 2
    count = len(shards)
    per_step = 8
    steps = perms // per_step
    once = pl.Buffered(1)
    whole = pl.BlockSpec((local, samples), lambda i: (0, 0), pipeline_mode=once)
    return pl.pallas_call(
        functools.partial(far_kernel, len(pairs), per_step),
        grid=(steps,),
        in_specs=[
            pl.BlockSpec((per_step * genes, samples), lambda i: (i + part * steps, 0)),
            pl.BlockSpec((perms, genes), lambda i: (before_part, 0), pipeline_mode=once),
            *[whole] * count,
            *[pl.BlockSpec((2, genes, local), lambda i, k=k: (k, 0, 0), pipeline_mode=once) for k in pairs],
        ],
        out_specs=pl.BlockSpec((perms, genes), lambda i: (0, 0)),
        out_shape=jax.ShapeDtypeStruct((perms, genes), jnp.float32),
        scratch_shapes=[pltpu.VMEM((2, per_step, genes, TILE // 2), jnp.float32)],
        cost_estimate=cost(2 * perms * genes * samples * count * local),
        compiler_params=params(24),
        name="far",
    )(table, before, *shards, *[masks] * len(pairs))


def finish_kernel(spread, best_ref, mate_ref, maxima_ref, sums_ref, *, samples):
    best = jnp.maximum(best_ref[...], mate_ref[...])
    maxima = best * best * samples
    maxima_ref[...] = maxima
    log_stat = jnp.log1p(maxima)
    sums = jnp.stack((jnp.sum(log_stat, axis=0), jnp.sum(log_stat * log_stat, axis=0)))
    sums_ref[...] = jnp.broadcast_to(sums[None], sums_ref.shape)


def finished(best, from_mate, samples, spread):
    perms, genes = best.shape
    return pl.pallas_call(
        functools.partial(finish_kernel, spread, samples=samples),
        out_shape=[
            jax.ShapeDtypeStruct((perms, genes), jnp.float32),
            jax.ShapeDtypeStruct((spread, 2, genes), jnp.float32),
        ],
        compiler_params=params(4),
        name="finish",
    )(best, from_mate)


def totals_kernel(sent_ref, moments_ref, pooled_ref):
    count, _, genes = sent_ref.shape
    blocks = lax.axis_size("gene")
    members = count // blocks
    mine = pl.multiple_of(lax.axis_index("gene") * members, members)
    moments_ref[...] = jnp.sum(sent_ref[pl.ds(mine, members)], axis=0) / PERMS
    every = jnp.sum(sent_ref[...], axis=0) / PERMS
    both = jnp.sum(every, axis=1, keepdims=True) / (genes * blocks)
    lane = lax.broadcasted_iota(jnp.int32, every.shape, 1)
    row = lax.broadcasted_iota(jnp.int32, every.shape, 0)
    spread = jnp.sum(jnp.where(lane == row, both, 0.0), axis=0, keepdims=True)
    pooled_ref[...] = spread[:, :2]


def totals(sent):
    return pl.pallas_call(
        totals_kernel,
        out_shape=[
            jax.ShapeDtypeStruct(sent.shape[1:], jnp.float32),
            jax.ShapeDtypeStruct((1, 2), jnp.float32),
        ],
        compiler_params=params(4),
        name="totals",
    )(sent)


def shards_program(genotypes, phenotypes, perm_rows, starts):
    var_n = lax.axis_size("var")
    rows_n = var_n // 2
    both = ("var", "perm")
    samples = phenotypes.shape[1]

    def along(step):
        return [(v, ((v // 2 + step) % rows_n) * 2 + v % 2) for v in range(var_n)]

    twin = [(v, v ^ 1) for v in range(var_n)]
    across = [(0, 1), (1, 0)]
    mate = [
        (v * 2 + z, ((((v // 2 + rows_n // 2) % rows_n) * 2 + v % 2) * 2 + 1 - z))
        for v in range(var_n) for z in range(2)
    ]

    mate_rows = lax.ppermute(perm_rows, both, mate)
    own = standard_rows(genotypes)
    below = lax.ppermute(own, "var", along(1))
    above = lax.ppermute(own, "var", along(-1))
    deep = lax.ppermute(own, "perm", across)
    own_twin = lax.ppermute(own, "var", twin)
    table, near, masks = near_best(phenotypes, perm_rows, mate_rows, starts, (own, own_twin))
    below, above, deep, masks = lax.optimization_barrier((below, above, deep, masks))
    far = [below, above, deep]
    far = far + [lax.ppermute(f, "var", twin) for f in far]
    to_mate = far_best(table, 1, near, 1, masks, (0,), far[:2])
    to_mate = far_best(table, 1, to_mate, 0, masks, (1, 2), far[2:])
    from_mate = lax.ppermute(to_mate, both, mate)
    best = far_best(table, 0, near, 0, masks, (0, 1, 2), far)
    count = lax.axis_size(("gene", "var", "perm"))
    maxima, sums = finished(best, from_mate, samples, count)

    sent = lax.all_to_all(sums, ("gene", "var", "perm"), 0, 0, tiled=True)
    moments, pooled = totals(sent)
    return (maxima, moments, pooled.reshape(2))


def solution(mesh):
    return jax.shard_map(
        shards_program,
        mesh=mesh,
        in_specs=(
            P("gene", ("var", "perm"), None),
            P("gene", None),
            P(("var", "perm"), None),
            P("gene"),
        ),
        out_specs=(P(("var", "perm"), "gene"), P(None, "gene"), P()),
        check_vma=False,
    )
```

```python
import functools

import jax
import jax.numpy as jnp
from jax import lax
from jax.experimental import pallas as pl
from jax.experimental.pallas import tpu as pltpu
from jax.sharding import PartitionSpec as P

WINDOW = 4096
PERMS = 256
FOLD = 256
TILE = 256
LARGE = 3.0e38


def standardized(values):
    centred = values - jnp.mean(values, axis=1, keepdims=True)
    inv_norm = lax.rsqrt(jnp.sum(centred * centred, axis=1, keepdims=True) + 1.0)
    return (centred * inv_norm).astype(jnp.bfloat16)


def cost(flops):
    return pl.CostEstimate(flops=flops, bytes_accessed=0, transcendentals=0)


def places(local):
    var_n, me, z = lax.axis_size("var"), lax.axis_index("var"), lax.axis_index("perm")
    rows_n = var_n // 2
    y, core = lax.div(me, 2), lax.rem(me, 2)

    def first(up, same_core, same_depth):
        c = core if same_core else 1 - core
        d = z if same_depth else 1 - z
        return ((lax.rem(y + up + rows_n, rows_n) * 2 + c) * 2 + d) * local

    near = [first(0, True, True), first(0, False, True)]
    far = [first(u, c, d) for c in (True, False) for u, d in ((-1, True), (1, True), (0, False))]
    return near, far


def window_mask(first, lead, width):
    half = TILE // 2
    lane = lax.broadcasted_iota(jnp.int32, lead.shape, 1)
    masks = []
    for r in range(0, width, half):
        past = lane + (first + r) - lead
        masks.append(jnp.where((past >= 0) & (past < WINDOW), LARGE, 0.0))
    return jnp.concatenate(masks, axis=1)


def weight_tiles(shards, local):
    half = TILE // 2
    pieces = [(i, r) for i in range(len(shards)) for r in range(0, local, half)]
    for t in range(0, len(pieces), 2):
        pair = pieces[t:t + 2]
        yield t * half, jnp.concatenate([shards[i][r:r + half, :] for i, r in pair], axis=0)


def lane_best(rows_bf16, shards, local, masks, copies):
    half = TILE // 2
    best = None
    for at, weights in weight_tiles(shards, local):
        scores = lax.dot_general(
            rows_bf16, weights, (((1,), (1,)), ((), ())), preferred_element_type=jnp.float32
        )
        for n in range(weights.shape[0] // half):
            i, r = divmod(at + n * half, local)
            mask_ref, k = masks[i]
            mask = mask_ref[k, :, r:r + half]
            part = jnp.abs(scores[:, n * half:(n + 1) * half]).reshape(copies, mask.shape[0], half)
            part = jnp.minimum(part, mask[None])
            best = part if best is None else jnp.maximum(best, part)
    return best


def reduce_lanes(best_ref, slot, out_ref, row):
    _, perms, genes, half = best_ref.shape
    lane = lax.broadcasted_iota(jnp.int32, (genes, half), 1)
    gene = lax.broadcasted_iota(jnp.int32, (genes, half), 0)
    for p in range(perms):
        top = jnp.max(best_ref[slot, p], axis=1, keepdims=True)
        best = jnp.max(jnp.where(lane == gene, top, 0.0), axis=0, keepdims=True)
        out_ref[pl.ds(row + p, 1), :] = best


def score_step(rows_bf16, shards, local, masks, per_step, best_ref, out_ref):
    step = pl.program_id(0)
    slot = lax.rem(step, 2)
    reduce_lanes(best_ref, 1 - slot, out_ref, jnp.maximum(step - 1, 0) * per_step)
    best_ref[slot] = lane_best(rows_bf16, shards, local, masks, per_step)

    @pl.when(step == pl.num_programs(0) - 1)
    def _():
        reduce_lanes(best_ref, slot, out_ref, step * per_step)


def near_kernel(per_step, base_ref, perm_ref, mate_ref, lead_ref, own_ref, twin_ref,
                table_ref, out_ref, far_mask_ref, rows_ref, mask_ref, best_ref):
    samples = own_ref.shape[1]
    folds = samples // FOLD
    genes = base_ref.shape[0] // folds
    local = own_ref.shape[0]
    half_perms = perm_ref.shape[0]
    step = pl.program_id(0)
    near_first, far_first = places(local)

    @pl.when(step == 0)
    def _():
        rows_ref[:half_perms, :] = perm_ref[...]
        rows_ref[half_perms:, :] = mate_ref[...]
        for i in range(2):
            mask_ref[i] = window_mask(near_first[i], lead_ref[...], local)

    shard = jnp.minimum(step, len(far_first) - 1)
    first = far_first[0]
    for i in range(1, len(far_first)):
        first = jnp.where(shard == i, far_first[i], first)
    far_mask_ref[shard] = window_mask(first, lead_ref[...], local)

    within = lax.broadcasted_iota(jnp.int32, (FOLD, samples), 0)
    for k in range(per_step):
        index = rows_ref[pl.ds(step * per_step + k, 1), :]
        low = jnp.bitwise_and(index, FOLD - 1)
        block = jnp.right_shift(index, FOLD.bit_length() - 1)
        hot = jnp.where(within == low, 1.0, 0.0).astype(jnp.bfloat16)
        picked = jnp.dot(base_ref[...], hot, preferred_element_type=jnp.float32)
        chosen = picked[:genes]
        for b in range(1, folds):
            chosen = jnp.where(block == b, picked[b * genes:(b + 1) * genes], chosen)
        table_ref[k * genes:(k + 1) * genes, :] = chosen.astype(jnp.bfloat16)
    masks = [(mask_ref, 0), (mask_ref, 1)]
    score_step(table_ref[...], (own_ref, twin_ref), local, masks, per_step, best_ref, out_ref)


def params(limit):
    return pltpu.CompilerParams(vmem_limit_bytes=limit * 1024 * 1024)


def in_hbm(array):
    return pltpu.with_memory_space_constraint(array, pltpu.HBM)


def head_kernel(x_ref, pheno_ref, perm_ref, starts_ref, own_ref, base_ref, rows_ref, lead_ref):
    own_ref[...] = standardized(x_ref[0].astype(jnp.float32))
    genes, samples = pheno_ref.shape
    std = standardized(pheno_ref[...])
    for b in range(samples // FOLD):
        base_ref[b * genes:(b + 1) * genes, :] = std[:, b * FOLD:(b + 1) * FOLD]
    rows_ref[...] = perm_ref[...]
    wide = jnp.broadcast_to(starts_ref[...].astype(jnp.float32), (lead_ref.shape[1], genes))
    lead_ref[...] = wide.T.astype(jnp.int32)


def head(genotypes, phenotypes, perm_rows, starts):
    _, local, samples = genotypes.shape
    genes = phenotypes.shape[0]
    inputs = (genotypes, phenotypes, perm_rows, starts.reshape(1, genes))
    return pl.pallas_call(
        head_kernel,
        out_shape=[
            jax.ShapeDtypeStruct((local, samples), jnp.bfloat16),
            jax.ShapeDtypeStruct((samples // FOLD * genes, FOLD), jnp.bfloat16),
            jax.ShapeDtypeStruct(perm_rows.shape, jnp.int32),
            jax.ShapeDtypeStruct((genes, TILE // 2), jnp.int32),
        ],
        cost_estimate=cost(8 * local * samples),
        compiler_params=params(16),
        name="head",
    )(*(in_hbm(i) for i in inputs))


def near_best(base, perm_rows, mate_rows, lead, shards):
    genes, samples = lead.shape[0], shards[0].shape[1]
    perms = perm_rows.shape[0] + mate_rows.shape[0]
    local = shards[0].shape[0]
    per_step = 4
    once = pl.Buffered(1)

    def whole(shape):
        return pl.BlockSpec(shape, lambda i: (0, 0), pipeline_mode=once)

    return pl.pallas_call(
        functools.partial(near_kernel, per_step),
        grid=(perms // per_step,),
        in_specs=[
            whole(base.shape),
            whole(perm_rows.shape),
            whole(mate_rows.shape),
            whole(lead.shape),
            whole((local, samples)),
            whole((local, samples)),
        ],
        out_specs=[
            pl.BlockSpec((per_step * genes, samples), lambda i: (i, 0)),
            pl.BlockSpec((perms, genes), lambda i: (0, 0)),
            pl.BlockSpec((6, genes, local), lambda i: (0, 0, 0)),
        ],
        out_shape=[
            jax.ShapeDtypeStruct((perms * genes, samples), jnp.bfloat16),
            jax.ShapeDtypeStruct((perms, genes), jnp.float32),
            jax.ShapeDtypeStruct((6, genes, local), jnp.float32),
        ],
        scratch_shapes=[
            pltpu.VMEM((perms, samples), jnp.int32),
            pltpu.VMEM((2, genes, local), jnp.float32),
            pltpu.VMEM((2, per_step, genes, TILE // 2), jnp.float32),
        ],
        cost_estimate=cost(2 * perms * genes * samples * (2 * local + samples)),
        compiler_params=params(24),
        name="near",
    )(base, perm_rows, mate_rows, lead, *shards)


def far_kernel(pairs, per_step, table_ref, before_ref, *refs):
    count = 2 * pairs
    shards, mask_refs, (out_ref, best_ref) = refs[:count], refs[count:count + pairs], refs[count + pairs:]
    local = shards[0].shape[0]
    masks = [(m, k) for m in mask_refs for k in range(2)]
    score_step(table_ref[...], shards, local, masks, per_step, best_ref, out_ref)

    @pl.when(pl.program_id(0) == pl.num_programs(0) - 1)
    def _():
        out_ref[...] = jnp.maximum(out_ref[...], before_ref[...])


def far_best(table, part, before, before_part, masks, pairs, shards):
    samples = table.shape[1]
    _, genes, local = masks.shape
    perms = table.shape[0] // genes // 2
    count = len(shards)
    per_step = 8
    steps = perms // per_step
    once = pl.Buffered(1)
    whole = pl.BlockSpec((local, samples), lambda i: (0, 0), pipeline_mode=once)
    return pl.pallas_call(
        functools.partial(far_kernel, len(pairs), per_step),
        grid=(steps,),
        in_specs=[
            pl.BlockSpec((per_step * genes, samples), lambda i: (i + part * steps, 0)),
            pl.BlockSpec((perms, genes), lambda i: (before_part, 0), pipeline_mode=once),
            *[whole] * count,
            *[pl.BlockSpec((2, genes, local), lambda i, k=k: (k, 0, 0), pipeline_mode=once) for k in pairs],
        ],
        out_specs=pl.BlockSpec((perms, genes), lambda i: (0, 0)),
        out_shape=jax.ShapeDtypeStruct((perms, genes), jnp.float32),
        scratch_shapes=[pltpu.VMEM((2, per_step, genes, TILE // 2), jnp.float32)],
        cost_estimate=cost(2 * perms * genes * samples * count * local),
        compiler_params=params(24),
        name="far",
    )(table, before, *shards, *[masks] * len(pairs))


def finish_kernel(best_ref, mate_ref, maxima_ref, sums_ref, *, samples):
    best = jnp.maximum(best_ref[...], mate_ref[...])
    maxima = best * best * samples
    maxima_ref[...] = maxima
    log_stat = jnp.log1p(maxima)
    sums = jnp.stack((jnp.sum(log_stat, axis=0), jnp.sum(log_stat * log_stat, axis=0)))
    sums_ref[...] = jnp.broadcast_to(sums[None], sums_ref.shape)


def finished(best, from_mate, samples, spread):
    perms, genes = best.shape
    return pl.pallas_call(
        functools.partial(finish_kernel, samples=samples),
        out_shape=[
            jax.ShapeDtypeStruct((perms, genes), jnp.float32),
            jax.ShapeDtypeStruct((spread, 2, genes), jnp.float32),
        ],
        compiler_params=params(4),
        name="finish",
    )(best, from_mate)


def totals_kernel(sent_ref, moments_ref, pooled_ref):
    count, _, genes = sent_ref.shape
    blocks = lax.axis_size("gene")
    members = count // blocks
    mine = pl.multiple_of(lax.axis_index("gene") * members, members)
    moments_ref[...] = jnp.sum(sent_ref[pl.ds(mine, members)], axis=0) / PERMS
    every = jnp.sum(sent_ref[...], axis=0) / PERMS
    both = jnp.sum(every, axis=1, keepdims=True) / (genes * blocks)
    lane = lax.broadcasted_iota(jnp.int32, every.shape, 1)
    row = lax.broadcasted_iota(jnp.int32, every.shape, 0)
    spread = jnp.sum(jnp.where(lane == row, both, 0.0), axis=0, keepdims=True)
    pooled_ref[...] = spread[:, :2]


def totals(sent):
    return pl.pallas_call(
        totals_kernel,
        out_shape=[
            jax.ShapeDtypeStruct(sent.shape[1:], jnp.float32),
            jax.ShapeDtypeStruct((1, 2), jnp.float32),
        ],
        compiler_params=params(4),
        name="totals",
    )(sent)


def shards_program(genotypes, phenotypes, perm_rows, starts):
    var_n = lax.axis_size("var")
    rows_n = var_n // 2
    both = ("var", "perm")
    samples = phenotypes.shape[1]

    def along(step):
        return [(v, ((v // 2 + step) % rows_n) * 2 + v % 2) for v in range(var_n)]

    twin = [(v, v ^ 1) for v in range(var_n)]
    across = [(0, 1), (1, 0)]
    mate = [
        (v * 2 + z, ((((v // 2 + rows_n // 2) % rows_n) * 2 + v % 2) * 2 + 1 - z))
        for v in range(var_n) for z in range(2)
    ]

    mate_rows = lax.ppermute(perm_rows, both, mate)
    own, base, own_rows, lead = head(genotypes, phenotypes, perm_rows, starts)
    deep = lax.ppermute(own, "perm", across)
    below = lax.ppermute(own, "var", along(1))
    above = lax.ppermute(own, "var", along(-1))
    own_twin = lax.ppermute(own, "var", twin)
    table, near, masks = near_best(base, own_rows, mate_rows, lead, (own, own_twin))
    below, above, deep, masks = lax.optimization_barrier((below, above, deep, masks))
    far = [below, above, deep]
    far = far + [lax.ppermute(f, "var", twin) for f in far]
    to_mate = far_best(table, 1, near, 1, masks, (0,), far[:2])
    to_mate = far_best(table, 1, to_mate, 0, masks, (1, 2), far[2:])
    from_mate = lax.ppermute(to_mate, both, mate)
    best = far_best(table, 0, near, 0, masks, (0, 1, 2), far)
    count = lax.axis_size(("gene", "var", "perm"))
    maxima, sums = finished(best, from_mate, samples, count)

    sent = lax.all_to_all(sums, ("gene", "var", "perm"), 0, 0, tiled=True)
    moments, pooled = totals(sent)
    return (maxima, moments, pooled.reshape(2))


def solution(mesh):
    return jax.shard_map(
        shards_program,
        mesh=mesh,
        in_specs=(
            P("gene", ("var", "perm"), None),
            P("gene", None),
            P(("var", "perm"), None),
            P("gene"),
        ),
        out_specs=(P(("var", "perm"), "gene"), P(None, "gene"), P()),
        check_vma=False,
    )
```

```python
import functools

import jax
import jax.numpy as jnp
from jax import lax
from jax.experimental import pallas as pl
from jax.experimental.pallas import tpu as pltpu
from jax.sharding import PartitionSpec as P

WINDOW = 4096
PERMS = 256
FOLD = 256
TILE = 256
LARGE = 3.0e38


def standardized(values):
    centred = values - jnp.mean(values, axis=1, keepdims=True)
    inv_norm = lax.rsqrt(jnp.sum(centred * centred, axis=1, keepdims=True) + 1.0)
    return (centred * inv_norm).astype(jnp.bfloat16)


def cost(flops):
    return pl.CostEstimate(flops=flops, bytes_accessed=0, transcendentals=0)


def places(local):
    var_n, me, z = lax.axis_size("var"), lax.axis_index("var"), lax.axis_index("perm")
    rows_n = var_n // 2
    y, core = lax.div(me, 2), lax.rem(me, 2)

    def first(up, same_core, same_depth):
        c = core if same_core else 1 - core
        d = z if same_depth else 1 - z
        return ((lax.rem(y + up + rows_n, rows_n) * 2 + c) * 2 + d) * local

    near = [first(0, True, True), first(0, False, True)]
    order = [(c, u, True) for c in (True, False) for u in (-1, 1)] + [(c, 0, False) for c in (True, False)]
    far = [first(u, c, d) for c, u, d in order]
    return near, far


def window_mask(first, lead, width):
    half = TILE // 2
    lane = lax.broadcasted_iota(jnp.int32, lead.shape, 1)
    masks = []
    for r in range(0, width, half):
        past = lane + (first + r) - lead
        masks.append(jnp.where((past >= 0) & (past < WINDOW), LARGE, 0.0))
    return jnp.concatenate(masks, axis=1)


def weight_tiles(shards, local):
    half = TILE // 2
    pieces = [(i, r) for i in range(len(shards)) for r in range(0, local, half)]
    for t in range(0, len(pieces), 2):
        pair = pieces[t:t + 2]
        yield t * half, jnp.concatenate([shards[i][r:r + half, :] for i, r in pair], axis=0)


def lane_best(rows_bf16, shards, local, masks, copies):
    half = TILE // 2
    best = None
    for at, weights in weight_tiles(shards, local):
        scores = lax.dot_general(
            rows_bf16, weights, (((1,), (1,)), ((), ())), preferred_element_type=jnp.float32
        )
        for n in range(weights.shape[0] // half):
            i, r = divmod(at + n * half, local)
            mask_ref, k = masks[i]
            mask = mask_ref[k, :, r:r + half]
            part = jnp.abs(scores[:, n * half:(n + 1) * half]).reshape(copies, mask.shape[0], half)
            part = jnp.minimum(part, mask[None])
            best = part if best is None else jnp.maximum(best, part)
    return best


def reduce_lanes(best_ref, slot, out_ref, row):
    _, perms, genes, half = best_ref.shape
    lane = lax.broadcasted_iota(jnp.int32, (genes, half), 1)
    gene = lax.broadcasted_iota(jnp.int32, (genes, half), 0)
    for p in range(perms):
        top = jnp.max(best_ref[slot, p], axis=1, keepdims=True)
        best = jnp.max(jnp.where(lane == gene, top, 0.0), axis=0, keepdims=True)
        out_ref[pl.ds(row + p, 1), :] = best


def score_step(rows_bf16, shards, local, masks, per_step, best_ref, out_ref):
    step = pl.program_id(0)
    slot = lax.rem(step, 2)
    reduce_lanes(best_ref, 1 - slot, out_ref, jnp.maximum(step - 1, 0) * per_step)
    best_ref[slot] = lane_best(rows_bf16, shards, local, masks, per_step)

    @pl.when(step == pl.num_programs(0) - 1)
    def _():
        reduce_lanes(best_ref, slot, out_ref, step * per_step)


def near_kernel(per_step, base_ref, perm_ref, mate_ref, lead_ref, own_ref, twin_ref,
                table_ref, out_ref, far_mask_ref, rows_ref, mask_ref, best_ref):
    samples = own_ref.shape[1]
    folds = samples // FOLD
    genes = base_ref.shape[0] // folds
    local = own_ref.shape[0]
    half_perms = perm_ref.shape[0]
    step = pl.program_id(0)
    near_first, far_first = places(local)

    @pl.when(step == 0)
    def _():
        rows_ref[:half_perms, :] = perm_ref[...]
        rows_ref[half_perms:, :] = mate_ref[...]
        for i in range(2):
            mask_ref[i] = window_mask(near_first[i], lead_ref[...], local)

    shard = jnp.minimum(step, len(far_first) - 1)
    first = far_first[0]
    for i in range(1, len(far_first)):
        first = jnp.where(shard == i, far_first[i], first)
    far_mask_ref[shard] = window_mask(first, lead_ref[...], local)

    within = lax.broadcasted_iota(jnp.int32, (FOLD, samples), 0)
    for k in range(per_step):
        index = rows_ref[pl.ds(step * per_step + k, 1), :]
        low = jnp.bitwise_and(index, FOLD - 1)
        block = jnp.right_shift(index, FOLD.bit_length() - 1)
        hot = jnp.where(within == low, 1.0, 0.0).astype(jnp.bfloat16)
        picked = jnp.dot(base_ref[...], hot, preferred_element_type=jnp.float32)
        chosen = picked[:genes]
        for b in range(1, folds):
            chosen = jnp.where(block == b, picked[b * genes:(b + 1) * genes], chosen)
        table_ref[k * genes:(k + 1) * genes, :] = chosen.astype(jnp.bfloat16)
    masks = [(mask_ref, 0), (mask_ref, 1)]
    score_step(table_ref[...], (own_ref, twin_ref), local, masks, per_step, best_ref, out_ref)


def params(limit):
    return pltpu.CompilerParams(vmem_limit_bytes=limit * 1024 * 1024)


def in_hbm(array):
    return pltpu.with_memory_space_constraint(array, pltpu.HBM)


def head_kernel(x_ref, pheno_ref, perm_ref, starts_ref, own_ref, base_ref, rows_ref, lead_ref):
    own_ref[...] = standardized(x_ref[0].astype(jnp.float32))
    genes, samples = pheno_ref.shape
    std = standardized(pheno_ref[...])
    for b in range(samples // FOLD):
        base_ref[b * genes:(b + 1) * genes, :] = std[:, b * FOLD:(b + 1) * FOLD]
    rows_ref[...] = perm_ref[...]
    wide = jnp.broadcast_to(starts_ref[...].astype(jnp.float32), (lead_ref.shape[1], genes))
    lead_ref[...] = wide.T.astype(jnp.int32)


def head(genotypes, phenotypes, perm_rows, starts):
    _, local, samples = genotypes.shape
    genes = phenotypes.shape[0]
    inputs = (genotypes, phenotypes, perm_rows, starts.reshape(1, genes))
    return pl.pallas_call(
        head_kernel,
        out_shape=[
            jax.ShapeDtypeStruct((local, samples), jnp.bfloat16),
            jax.ShapeDtypeStruct((samples // FOLD * genes, FOLD), jnp.bfloat16),
            jax.ShapeDtypeStruct(perm_rows.shape, jnp.int32),
            jax.ShapeDtypeStruct((genes, TILE // 2), jnp.int32),
        ],
        cost_estimate=cost(8 * local * samples),
        compiler_params=params(16),
        name="head",
    )(*(in_hbm(i) for i in inputs))


def near_best(base, perm_rows, mate_rows, lead, shards):
    genes, samples = lead.shape[0], shards[0].shape[1]
    perms = perm_rows.shape[0] + mate_rows.shape[0]
    local = shards[0].shape[0]
    per_step = 4
    once = pl.Buffered(1)

    def whole(shape):
        return pl.BlockSpec(shape, lambda i: (0, 0), pipeline_mode=once)

    return pl.pallas_call(
        functools.partial(near_kernel, per_step),
        grid=(perms // per_step,),
        in_specs=[
            whole(base.shape),
            whole(perm_rows.shape),
            whole(mate_rows.shape),
            whole(lead.shape),
            whole((local, samples)),
            whole((local, samples)),
        ],
        out_specs=[
            pl.BlockSpec((per_step * genes, samples), lambda i: (i, 0)),
            pl.BlockSpec((perms, genes), lambda i: (0, 0)),
            pl.BlockSpec((6, genes, local), lambda i: (0, 0, 0)),
        ],
        out_shape=[
            jax.ShapeDtypeStruct((perms * genes, samples), jnp.bfloat16),
            jax.ShapeDtypeStruct((perms, genes), jnp.float32),
            jax.ShapeDtypeStruct((6, genes, local), jnp.float32),
        ],
        scratch_shapes=[
            pltpu.VMEM((perms, samples), jnp.int32),
            pltpu.VMEM((2, genes, local), jnp.float32),
            pltpu.VMEM((2, per_step, genes, TILE // 2), jnp.float32),
        ],
        cost_estimate=cost(2 * perms * genes * samples * (2 * local + samples)),
        compiler_params=params(24),
        name="near",
    )(base, perm_rows, mate_rows, lead, *shards)


def far_kernel(pairs, per_step, table_ref, before_ref, *refs):
    count = 2 * pairs
    shards, mask_refs, (out_ref, best_ref) = refs[:count], refs[count:count + pairs], refs[count + pairs:]
    local = shards[0].shape[0]
    masks = [(m, k) for m in mask_refs for k in range(2)]
    score_step(table_ref[...], shards, local, masks, per_step, best_ref, out_ref)

    @pl.when(pl.program_id(0) == pl.num_programs(0) - 1)
    def _():
        out_ref[...] = jnp.maximum(out_ref[...], before_ref[...])


def far_best(table, part, before, before_part, masks, pairs, shards):
    samples = table.shape[1]
    _, genes, local = masks.shape
    perms = table.shape[0] // genes // 2
    count = len(shards)
    per_step = perms if count == 2 else 8
    steps = perms // per_step
    once = pl.Buffered(1)
    whole = pl.BlockSpec((local, samples), lambda i: (0, 0), pipeline_mode=once)
    return pl.pallas_call(
        functools.partial(far_kernel, len(pairs), per_step),
        grid=(steps,),
        in_specs=[
            pl.BlockSpec((per_step * genes, samples), lambda i: (i + part * steps, 0)),
            pl.BlockSpec((perms, genes), lambda i: (before_part, 0), pipeline_mode=once),
            *[whole] * count,
            *[pl.BlockSpec((2, genes, local), lambda i, k=k: (k, 0, 0), pipeline_mode=once) for k in pairs],
        ],
        out_specs=pl.BlockSpec((perms, genes), lambda i: (0, 0)),
        out_shape=jax.ShapeDtypeStruct((perms, genes), jnp.float32),
        scratch_shapes=[pltpu.VMEM((2, per_step, genes, TILE // 2), jnp.float32)],
        cost_estimate=cost(2 * perms * genes * samples * count * local),
        compiler_params=params(24),
        name="far",
    )(table, before, *shards, *[masks] * len(pairs))


def finish_kernel(best_ref, mate_ref, maxima_ref, sums_ref, *, samples):
    best = jnp.maximum(best_ref[...], mate_ref[...])
    maxima = best * best * samples
    maxima_ref[...] = maxima
    log_stat = jnp.log1p(maxima)
    sums = jnp.stack((jnp.sum(log_stat, axis=0), jnp.sum(log_stat * log_stat, axis=0)))
    sums_ref[...] = jnp.broadcast_to(sums[None], sums_ref.shape)


def finished(best, from_mate, samples, spread):
    perms, genes = best.shape
    return pl.pallas_call(
        functools.partial(finish_kernel, samples=samples),
        out_shape=[
            jax.ShapeDtypeStruct((perms, genes), jnp.float32),
            jax.ShapeDtypeStruct((spread, 2, genes), jnp.float32),
        ],
        compiler_params=params(4),
        name="finish",
    )(best, from_mate)


def totals_kernel(sent_ref, moments_ref, pooled_ref):
    count, _, genes = sent_ref.shape
    blocks = lax.axis_size("gene")
    members = count // blocks
    mine = pl.multiple_of(lax.axis_index("gene") * members, members)
    moments_ref[...] = jnp.sum(sent_ref[pl.ds(mine, members)], axis=0) / PERMS
    every = jnp.sum(sent_ref[...], axis=0) / PERMS
    both = jnp.sum(every, axis=1, keepdims=True) / (genes * blocks)
    lane = lax.broadcasted_iota(jnp.int32, every.shape, 1)
    row = lax.broadcasted_iota(jnp.int32, every.shape, 0)
    spread = jnp.sum(jnp.where(lane == row, both, 0.0), axis=0, keepdims=True)
    pooled_ref[...] = spread[:, :2]


def totals(sent):
    return pl.pallas_call(
        totals_kernel,
        out_shape=[
            jax.ShapeDtypeStruct(sent.shape[1:], jnp.float32),
            jax.ShapeDtypeStruct((1, 2), jnp.float32),
        ],
        compiler_params=params(4),
        name="totals",
    )(sent)


def shards_program(genotypes, phenotypes, perm_rows, starts):
    var_n = lax.axis_size("var")
    rows_n = var_n // 2
    both = ("var", "perm")
    samples = phenotypes.shape[1]

    def along(step):
        return [(v, ((v // 2 + step) % rows_n) * 2 + v % 2) for v in range(var_n)]

    twin = [(v, v ^ 1) for v in range(var_n)]
    across = [(0, 1), (1, 0)]
    mate = [
        (v * 2 + z, ((((v // 2 + rows_n // 2) % rows_n) * 2 + v % 2) * 2 + 1 - z))
        for v in range(var_n) for z in range(2)
    ]

    mate_rows = lax.ppermute(perm_rows, both, mate)
    own, base, own_rows, lead = head(genotypes, phenotypes, perm_rows, starts)
    deep = lax.ppermute(own, "perm", across)
    below = lax.ppermute(own, "var", along(1))
    above = lax.ppermute(own, "var", along(-1))
    own_twin = lax.ppermute(own, "var", twin)
    table, near, masks = near_best(base, own_rows, mate_rows, lead, (own, own_twin))
    below, above, masks = lax.optimization_barrier((below, above, masks))
    below_twin = lax.ppermute(below, "var", twin)
    above_twin = lax.ppermute(above, "var", twin)
    to_mate = far_best(table, 1, near, 1, masks, (0,), [below, above])
    deep, to_mate = lax.optimization_barrier((deep, to_mate))
    deep_twin = lax.ppermute(deep, "var", twin)
    to_mate = far_best(table, 1, to_mate, 0, masks, (1,), [below_twin, above_twin])
    to_mate = far_best(table, 1, to_mate, 0, masks, (2,), [deep, deep_twin])
    from_mate = lax.ppermute(to_mate, both, mate)
    far = [below, above, below_twin, above_twin, deep, deep_twin]
    best = far_best(table, 0, near, 0, masks, (0, 1, 2), far)
    count = lax.axis_size(("gene", "var", "perm"))
    maxima, sums = finished(best, from_mate, samples, count)

    sent = lax.all_to_all(sums, ("gene", "var", "perm"), 0, 0, tiled=True)
    moments, pooled = totals(sent)
    return (maxima, moments, pooled.reshape(2))


def solution(mesh):
    return jax.shard_map(
        shards_program,
        mesh=mesh,
        in_specs=(
            P("gene", ("var", "perm"), None),
            P("gene", None),
            P(("var", "perm"), None),
            P("gene"),
        ),
        out_specs=(P(("var", "perm"), "gene"), P(None, "gene"), P()),
        check_vma=False,
    )
```

```python
import functools

import jax
import jax.numpy as jnp
from jax import lax
from jax.experimental import pallas as pl
from jax.experimental.pallas import tpu as pltpu
from jax.sharding import PartitionSpec as P

WINDOW = 4096
PERMS = 256
FOLD = 256
TILE = 256
LARGE = 3.0e38


def standardized(values):
    centred = values - jnp.mean(values, axis=1, keepdims=True)
    inv_norm = lax.rsqrt(jnp.sum(centred * centred, axis=1, keepdims=True) + 1.0)
    return (centred * inv_norm).astype(jnp.bfloat16)


def cost(flops):
    return pl.CostEstimate(flops=flops, bytes_accessed=0, transcendentals=0)


def places(local):
    var_n, me, z = lax.axis_size("var"), lax.axis_index("var"), lax.axis_index("perm")
    rows_n = var_n // 2
    y, core = lax.div(me, 2), lax.rem(me, 2)

    def first(up, same_core, same_depth):
        c = core if same_core else 1 - core
        d = z if same_depth else 1 - z
        return ((lax.rem(y + up + rows_n, rows_n) * 2 + c) * 2 + d) * local

    near = [first(0, True, True), first(0, False, True)]
    order = [(c, u, True) for c in (True, False) for u in (-1, 1)] + [(c, 0, False) for c in (True, False)]
    far = [first(u, c, d) for c, u, d in order]
    return near, far


def window_mask(first, lead, width):
    half = TILE // 2
    lane = lax.broadcasted_iota(jnp.int32, lead.shape, 1)
    masks = []
    for r in range(0, width, half):
        past = lane + (first + r) - lead
        masks.append(jnp.where((past >= 0) & (past < WINDOW), LARGE, 0.0))
    return jnp.concatenate(masks, axis=1)


def weight_tiles(shards, local):
    half = TILE // 2
    pieces = [(i, r) for i in range(len(shards)) for r in range(0, local, half)]
    for t in range(0, len(pieces), 2):
        pair = pieces[t:t + 2]
        yield t * half, jnp.concatenate([shards[i][r:r + half, :] for i, r in pair], axis=0)


def lane_best(rows_bf16, shards, local, masks, copies):
    half = TILE // 2
    best = None
    for at, weights in weight_tiles(shards, local):
        scores = lax.dot_general(
            rows_bf16, weights, (((1,), (1,)), ((), ())), preferred_element_type=jnp.float32
        )
        for n in range(weights.shape[0] // half):
            i, r = divmod(at + n * half, local)
            mask_ref, k = masks[i]
            mask = mask_ref[k, :, r:r + half]
            part = jnp.abs(scores[:, n * half:(n + 1) * half]).reshape(copies, mask.shape[0], half)
            part = jnp.minimum(part, mask[None])
            best = part if best is None else jnp.maximum(best, part)
    return best


def reduce_lanes(best_ref, slot, out_ref, row):
    _, perms, genes, half = best_ref.shape
    lane = lax.broadcasted_iota(jnp.int32, (genes, half), 1)
    gene = lax.broadcasted_iota(jnp.int32, (genes, half), 0)
    for p in range(perms):
        top = jnp.max(best_ref[slot, p], axis=1, keepdims=True)
        best = jnp.max(jnp.where(lane == gene, top, 0.0), axis=0, keepdims=True)
        out_ref[pl.ds(row + p, 1), :] = best


def score_step(rows_bf16, shards, local, masks, per_step, best_ref, out_ref):
    step = pl.program_id(0)
    slot = lax.rem(step, 2)
    reduce_lanes(best_ref, 1 - slot, out_ref, jnp.maximum(step - 1, 0) * per_step)
    best_ref[slot] = lane_best(rows_bf16, shards, local, masks, per_step)

    @pl.when(step == pl.num_programs(0) - 1)
    def _():
        reduce_lanes(best_ref, slot, out_ref, step * per_step)


def near_kernel(per_step, base_ref, perm_ref, mate_ref, lead_ref, own_ref, twin_ref,
                table_ref, out_ref, far_mask_ref, rows_ref, mask_ref, best_ref):
    samples = own_ref.shape[1]
    folds = samples // FOLD
    genes = base_ref.shape[0] // folds
    local = own_ref.shape[0]
    half_perms = perm_ref.shape[0]
    step = pl.program_id(0)
    near_first, far_first = places(local)

    @pl.when(step == 0)
    def _():
        rows_ref[:half_perms, :] = perm_ref[...]
        rows_ref[half_perms:, :] = mate_ref[...]
        for i in range(2):
            mask_ref[i] = window_mask(near_first[i], lead_ref[...], local)

    shard = jnp.minimum(step, len(far_first) - 1)
    first = far_first[0]
    for i in range(1, len(far_first)):
        first = jnp.where(shard == i, far_first[i], first)
    far_mask_ref[shard] = window_mask(first, lead_ref[...], local)

    within = lax.broadcasted_iota(jnp.int32, (FOLD, samples), 0)
    for k in range(per_step):
        index = rows_ref[pl.ds(step * per_step + k, 1), :]
        low = jnp.bitwise_and(index, FOLD - 1)
        block = jnp.right_shift(index, FOLD.bit_length() - 1)
        hot = jnp.where(within == low, 1.0, 0.0).astype(jnp.bfloat16)
        picked = jnp.dot(base_ref[...], hot, preferred_element_type=jnp.float32)
        chosen = picked[:genes]
        for b in range(1, folds):
            chosen = jnp.where(block == b, picked[b * genes:(b + 1) * genes], chosen)
        table_ref[k * genes:(k + 1) * genes, :] = chosen.astype(jnp.bfloat16)
    masks = [(mask_ref, 0), (mask_ref, 1)]
    score_step(table_ref[...], (own_ref, twin_ref), local, masks, per_step, best_ref, out_ref)


def params(limit):
    return pltpu.CompilerParams(vmem_limit_bytes=limit * 1024 * 1024)


def in_hbm(array):
    return pltpu.with_memory_space_constraint(array, pltpu.HBM)


def head_kernel(x_ref, pheno_ref, perm_ref, starts_ref, own_ref, base_ref, rows_ref, lead_ref):
    own_ref[...] = standardized(x_ref[0].astype(jnp.float32))
    genes, samples = pheno_ref.shape
    std = standardized(pheno_ref[...])
    for b in range(samples // FOLD):
        base_ref[b * genes:(b + 1) * genes, :] = std[:, b * FOLD:(b + 1) * FOLD]
    rows_ref[...] = perm_ref[...]
    wide = jnp.broadcast_to(starts_ref[...].astype(jnp.float32), (lead_ref.shape[1], genes))
    lead_ref[...] = wide.T.astype(jnp.int32)


def head(genotypes, phenotypes, perm_rows, starts):
    _, local, samples = genotypes.shape
    genes = phenotypes.shape[0]
    inputs = (genotypes, phenotypes, perm_rows, starts.reshape(1, genes))
    return pl.pallas_call(
        head_kernel,
        out_shape=[
            jax.ShapeDtypeStruct((local, samples), jnp.bfloat16),
            jax.ShapeDtypeStruct((samples // FOLD * genes, FOLD), jnp.bfloat16),
            jax.ShapeDtypeStruct(perm_rows.shape, jnp.int32),
            jax.ShapeDtypeStruct((genes, TILE // 2), jnp.int32),
        ],
        cost_estimate=cost(8 * local * samples),
        compiler_params=params(16),
        name="head",
    )(*(in_hbm(i) for i in inputs))


def near_best(base, perm_rows, mate_rows, lead, shards):
    genes, samples = lead.shape[0], shards[0].shape[1]
    perms = perm_rows.shape[0] + mate_rows.shape[0]
    local = shards[0].shape[0]
    per_step = 4
    once = pl.Buffered(1)

    def whole(shape):
        return pl.BlockSpec(shape, lambda i: (0, 0), pipeline_mode=once)

    return pl.pallas_call(
        functools.partial(near_kernel, per_step),
        grid=(perms // per_step,),
        in_specs=[
            whole(base.shape),
            whole(perm_rows.shape),
            whole(mate_rows.shape),
            whole(lead.shape),
            whole((local, samples)),
            whole((local, samples)),
        ],
        out_specs=[
            pl.BlockSpec((per_step * genes, samples), lambda i: (i, 0)),
            pl.BlockSpec((perms, genes), lambda i: (0, 0)),
            pl.BlockSpec((6, genes, local), lambda i: (0, 0, 0)),
        ],
        out_shape=[
            jax.ShapeDtypeStruct((perms * genes, samples), jnp.bfloat16),
            jax.ShapeDtypeStruct((perms, genes), jnp.float32),
            jax.ShapeDtypeStruct((6, genes, local), jnp.float32),
        ],
        scratch_shapes=[
            pltpu.VMEM((perms, samples), jnp.int32),
            pltpu.VMEM((2, genes, local), jnp.float32),
            pltpu.VMEM((2, per_step, genes, TILE // 2), jnp.float32),
        ],
        cost_estimate=cost(2 * perms * genes * samples * (2 * local + samples)),
        compiler_params=params(24),
        name="near",
    )(base, perm_rows, mate_rows, lead, *shards)


def reduced(best):
    perms, genes, half = best.shape
    lane = lax.broadcasted_iota(jnp.int32, (genes, half), 1)
    gene = lax.broadcasted_iota(jnp.int32, (genes, half), 0)
    rows = []
    for p in range(perms):
        top = jnp.max(best[p], axis=1, keepdims=True)
        rows.append(jnp.max(jnp.where(lane == gene, top, 0.0), axis=0, keepdims=True))
    return jnp.concatenate(rows, axis=0)


def far_kernel(start, close, table_ref, near_ref, mask_ref, one_ref, two_ref, *refs):
    genes = near_ref.shape[1]
    local = one_ref.shape[0]
    copies = table_ref.shape[0] // genes
    best = lane_best(
        table_ref[...], (one_ref, two_ref), local, [(mask_ref, 0), (mask_ref, 1)], copies
    )
    refs = list(refs)
    if not start:
        best = jnp.maximum(best, refs.pop(0)[...])
    if close == "none":
        refs[0][...] = best
        return
    top = jnp.maximum(reduced(best), near_ref[...])
    if close == "send":
        refs[0][...] = top
        return
    mate_ref, maxima_ref, sums_ref = refs
    top = jnp.maximum(top, mate_ref[...])
    maxima = top * top * one_ref.shape[1]
    maxima_ref[...] = maxima
    log_stat = jnp.log1p(maxima)
    sums = jnp.stack((jnp.sum(log_stat, axis=0), jnp.sum(log_stat * log_stat, axis=0)))
    sums_ref[...] = jnp.broadcast_to(sums[None], sums_ref.shape)


def far_best(table, part, near, masks, pair, shards, carried=None, close="none", from_mate=None, spread=0):
    samples = table.shape[1]
    _, genes, local = masks.shape
    perms = table.shape[0] // genes // 2
    rows = perms * genes
    wide = (perms, genes, TILE // 2)
    once = pl.Buffered(1)

    def whole(shape):
        return pl.BlockSpec(shape, lambda i: (0,) * len(shape), pipeline_mode=once)

    extra = [x for x in (carried, from_mate) if x is not None]
    shape = {
        "none": [wide], "send": [(perms, genes)], "finish": [(perms, genes), (spread, 2, genes)]
    }[close]
    out = pl.pallas_call(
        functools.partial(far_kernel, carried is None, close),
        grid=(1,),
        in_specs=[
            pl.BlockSpec((rows, samples), lambda i: (part, 0), pipeline_mode=once),
            pl.BlockSpec((perms, genes), lambda i: (part, 0), pipeline_mode=once),
            pl.BlockSpec((2, genes, local), lambda i: (pair, 0, 0), pipeline_mode=once),
            whole((local, samples)),
            whole((local, samples)),
            *[whole(x.shape) for x in extra],
        ],
        out_specs=[whole(x) for x in shape],
        out_shape=[jax.ShapeDtypeStruct(x, jnp.float32) for x in shape],
        cost_estimate=cost(2 * rows * samples * 2 * local),
        compiler_params=params(24),
        name="far",
    )(table, near, masks, *shards, *extra)
    return out if len(out) > 1 else out[0]


def totals_kernel(sent_ref, moments_ref, pooled_ref):
    count, _, genes = sent_ref.shape
    blocks = lax.axis_size("gene")
    members = count // blocks
    mine = pl.multiple_of(lax.axis_index("gene") * members, members)
    moments_ref[...] = jnp.sum(sent_ref[pl.ds(mine, members)], axis=0) / PERMS
    every = jnp.sum(sent_ref[...], axis=0) / PERMS
    both = jnp.sum(every, axis=1, keepdims=True) / (genes * blocks)
    lane = lax.broadcasted_iota(jnp.int32, every.shape, 1)
    row = lax.broadcasted_iota(jnp.int32, every.shape, 0)
    spread = jnp.sum(jnp.where(lane == row, both, 0.0), axis=0, keepdims=True)
    pooled_ref[...] = spread[:, :2]


def totals(sent):
    return pl.pallas_call(
        totals_kernel,
        out_shape=[
            jax.ShapeDtypeStruct(sent.shape[1:], jnp.float32),
            jax.ShapeDtypeStruct((1, 2), jnp.float32),
        ],
        compiler_params=params(4),
        name="totals",
    )(sent)


def shards_program(genotypes, phenotypes, perm_rows, starts):
    var_n = lax.axis_size("var")
    rows_n = var_n // 2
    both = ("var", "perm")

    def along(step):
        return [(v, ((v // 2 + step) % rows_n) * 2 + v % 2) for v in range(var_n)]

    twin = [(v, v ^ 1) for v in range(var_n)]
    across = [(0, 1), (1, 0)]
    mate = [
        (v * 2 + z, ((((v // 2 + rows_n // 2) % rows_n) * 2 + v % 2) * 2 + 1 - z))
        for v in range(var_n) for z in range(2)
    ]

    mate_rows = lax.ppermute(perm_rows, both, mate)
    own, base, own_rows, lead = head(genotypes, phenotypes, perm_rows, starts)
    deep = lax.ppermute(own, "perm", across)
    below = lax.ppermute(own, "var", along(1))
    above = lax.ppermute(own, "var", along(-1))
    own_twin = lax.ppermute(own, "var", twin)
    table, near, masks = near_best(base, own_rows, mate_rows, lead, (own, own_twin))
    below, above, masks = lax.optimization_barrier((below, above, masks))
    below_twin = lax.ppermute(below, "var", twin)
    above_twin = lax.ppermute(above, "var", twin)
    lanes = far_best(table, 1, near, masks, 0, (below, above))
    deep, lanes = lax.optimization_barrier((deep, lanes))
    deep_twin = lax.ppermute(deep, "var", twin)
    lanes = far_best(table, 1, near, masks, 1, (below_twin, above_twin), lanes)
    to_mate = far_best(table, 1, near, masks, 2, (deep, deep_twin), lanes, "send")
    from_mate = lax.ppermute(to_mate, both, mate)
    lanes = far_best(table, 0, near, masks, 0, (below, above))
    lanes = far_best(table, 0, near, masks, 1, (below_twin, above_twin), lanes)
    count = lax.axis_size(("gene", "var", "perm"))
    maxima, sums = far_best(
        table, 0, near, masks, 2, (deep, deep_twin), lanes, "finish", from_mate, count
    )

    sent = lax.all_to_all(sums, ("gene", "var", "perm"), 0, 0, tiled=True)
    moments, pooled = totals(sent)
    return (maxima, moments, pooled.reshape(2))


def solution(mesh):
    return jax.shard_map(
        shards_program,
        mesh=mesh,
        in_specs=(
            P("gene", ("var", "perm"), None),
            P("gene", None),
            P(("var", "perm"), None),
            P("gene"),
        ),
        out_specs=(P(("var", "perm"), "gene"), P(None, "gene"), P()),
        check_vma=False,
    )
```

```python
import functools

import jax
import jax.numpy as jnp
from jax import lax
from jax.experimental import pallas as pl
from jax.experimental.pallas import tpu as pltpu
from jax.sharding import PartitionSpec as P

WINDOW = 4096
PERMS = 256
FOLD = 256
TILE = 256
LARGE = 3.0e38
CHUNK = 4


def standardized(values):
    centred = values - jnp.mean(values, axis=1, keepdims=True)
    inv_norm = lax.rsqrt(jnp.sum(centred * centred, axis=1, keepdims=True) + 1.0)
    return (centred * inv_norm).astype(jnp.bfloat16)


def cost(flops):
    return pl.CostEstimate(flops=flops, bytes_accessed=0, transcendentals=0)


def places(local):
    var_n, me, z = lax.axis_size("var"), lax.axis_index("var"), lax.axis_index("perm")
    rows_n = var_n // 2
    y, core = lax.div(me, 2), lax.rem(me, 2)

    def first(up, same_core, same_depth):
        c = core if same_core else 1 - core
        d = z if same_depth else 1 - z
        return ((lax.rem(y + up + rows_n, rows_n) * 2 + c) * 2 + d) * local

    near = [first(0, True, True), first(0, False, True)]
    order = [(c, u, True) for c in (True, False) for u in (-1, 1)] + [(c, 0, False) for c in (True, False)]
    far = [first(u, c, d) for c, u, d in order]
    return near, far


def window_mask(first, lead, width):
    half = TILE // 2
    lane = lax.broadcasted_iota(jnp.int32, lead.shape, 1)
    masks = []
    for r in range(0, width, half):
        past = lane + (first + r) - lead
        masks.append(jnp.where((past >= 0) & (past < WINDOW), LARGE, 0.0))
    return jnp.concatenate(masks, axis=1)


def weight_tiles(shards, local):
    half = TILE // 2
    pieces = [(i, r) for i in range(len(shards)) for r in range(0, local, half)]
    for t in range(0, len(pieces), 2):
        pair = pieces[t:t + 2]
        yield t * half, jnp.concatenate([shards[i][r:r + half, :] for i, r in pair], axis=0)


def lane_best(rows_bf16, shards, local, masks, copies):
    half = TILE // 2
    best = None
    for at, weights in weight_tiles(shards, local):
        scores = lax.dot_general(
            rows_bf16, weights, (((1,), (1,)), ((), ())), preferred_element_type=jnp.float32
        )
        for n in range(weights.shape[0] // half):
            i, r = divmod(at + n * half, local)
            mask_ref, k = masks[i]
            mask = mask_ref[k, :, r:r + half]
            part = jnp.abs(scores[:, n * half:(n + 1) * half]).reshape(copies, mask.shape[0], half)
            part = jnp.minimum(part, mask[None])
            best = part if best is None else jnp.maximum(best, part)
    return best


def reduce_lanes(best_ref, slot, out_ref, row):
    _, perms, genes, half = best_ref.shape
    lane = lax.broadcasted_iota(jnp.int32, (genes, half), 1)
    gene = lax.broadcasted_iota(jnp.int32, (genes, half), 0)
    for p in range(perms):
        top = jnp.max(best_ref[slot, p], axis=1, keepdims=True)
        best = jnp.max(jnp.where(lane == gene, top, 0.0), axis=0, keepdims=True)
        out_ref[pl.ds(row + p, 1), :] = best


def score_step(rows_bf16, shards, local, masks, per_step, best_ref, out_ref):
    step = pl.program_id(0)
    slot = lax.rem(step, 2)
    reduce_lanes(best_ref, 1 - slot, out_ref, jnp.maximum(step - 1, 0) * per_step)
    best_ref[slot] = lane_best(rows_bf16, shards, local, masks, per_step)

    @pl.when(step == pl.num_programs(0) - 1)
    def _():
        reduce_lanes(best_ref, slot, out_ref, step * per_step)


def near_kernel(per_step, base_ref, perm_ref, mate_ref, lead_ref, own_ref, twin_ref,
                table_ref, out_ref, far_mask_ref, rows_ref, mask_ref, best_ref):
    samples = own_ref.shape[1]
    folds = samples // FOLD
    genes = base_ref.shape[0] // folds
    local = own_ref.shape[0]
    half_perms = perm_ref.shape[0]
    step = pl.program_id(0)
    near_first, far_first = places(local)

    @pl.when(step == 0)
    def _():
        rows_ref[:half_perms, :] = perm_ref[...]
        rows_ref[half_perms:, :] = mate_ref[...]
        for i in range(2):
            mask_ref[i] = window_mask(near_first[i], lead_ref[...], local)

    shard = jnp.minimum(step, len(far_first) - 1)
    first = far_first[0]
    for i in range(1, len(far_first)):
        first = jnp.where(shard == i, far_first[i], first)
    far_mask_ref[shard] = window_mask(first, lead_ref[...], local)

    within = lax.broadcasted_iota(jnp.int32, (FOLD, samples), 0)
    for k in range(per_step):
        index = rows_ref[pl.ds(step * per_step + k, 1), :]
        low = jnp.bitwise_and(index, FOLD - 1)
        block = jnp.right_shift(index, FOLD.bit_length() - 1)
        hot = jnp.where(within == low, 1.0, 0.0).astype(jnp.bfloat16)
        picked = jnp.dot(base_ref[...], hot, preferred_element_type=jnp.float32)
        chosen = picked[:genes]
        for b in range(1, folds):
            chosen = jnp.where(block == b, picked[b * genes:(b + 1) * genes], chosen)
        table_ref[k * genes:(k + 1) * genes, :] = chosen.astype(jnp.bfloat16)
    masks = [(mask_ref, 0), (mask_ref, 1)]
    score_step(table_ref[...], (own_ref, twin_ref), local, masks, per_step, best_ref, out_ref)


def params(limit):
    return pltpu.CompilerParams(vmem_limit_bytes=limit * 1024 * 1024)


def in_hbm(array):
    return pltpu.with_memory_space_constraint(array, pltpu.HBM)


def head_kernel(x_ref, pheno_ref, perm_ref, starts_ref, own_ref, base_ref, rows_ref, lead_ref):
    own_ref[...] = standardized(x_ref[0].astype(jnp.float32))
    genes, samples = pheno_ref.shape
    std = standardized(pheno_ref[...])
    for b in range(samples // FOLD):
        base_ref[b * genes:(b + 1) * genes, :] = std[:, b * FOLD:(b + 1) * FOLD]
    rows_ref[...] = perm_ref[...]
    wide = jnp.broadcast_to(starts_ref[...].astype(jnp.float32), (lead_ref.shape[1], genes))
    lead_ref[...] = wide.T.astype(jnp.int32)


def head(genotypes, phenotypes, perm_rows, starts):
    _, local, samples = genotypes.shape
    genes = phenotypes.shape[0]
    inputs = (genotypes, phenotypes, perm_rows, starts.reshape(1, genes))
    return pl.pallas_call(
        head_kernel,
        out_shape=[
            jax.ShapeDtypeStruct((local, samples), jnp.bfloat16),
            jax.ShapeDtypeStruct((samples // FOLD * genes, FOLD), jnp.bfloat16),
            jax.ShapeDtypeStruct(perm_rows.shape, jnp.int32),
            jax.ShapeDtypeStruct((genes, TILE // 2), jnp.int32),
        ],
        cost_estimate=cost(8 * local * samples),
        compiler_params=params(16),
        name="head",
    )(*(in_hbm(i) for i in inputs))


def near_best(base, perm_rows, mate_rows, lead, shards):
    genes, samples = lead.shape[0], shards[0].shape[1]
    perms = perm_rows.shape[0] + mate_rows.shape[0]
    local = shards[0].shape[0]
    per_step = 4
    once = pl.Buffered(1)

    def whole(shape):
        return pl.BlockSpec(shape, lambda i: (0, 0), pipeline_mode=once)

    return pl.pallas_call(
        functools.partial(near_kernel, per_step),
        grid=(perms // per_step,),
        in_specs=[
            whole(base.shape),
            whole(perm_rows.shape),
            whole(mate_rows.shape),
            whole(lead.shape),
            whole((local, samples)),
            whole((local, samples)),
        ],
        out_specs=[
            pl.BlockSpec((per_step * genes, samples), lambda i: (i, 0)),
            pl.BlockSpec((perms, genes), lambda i: (0, 0)),
            pl.BlockSpec((6, genes, local), lambda i: (0, 0, 0)),
        ],
        out_shape=[
            jax.ShapeDtypeStruct((perms * genes, samples), jnp.bfloat16),
            jax.ShapeDtypeStruct((perms, genes), jnp.float32),
            jax.ShapeDtypeStruct((6, genes, local), jnp.float32),
        ],
        scratch_shapes=[
            pltpu.VMEM((perms, samples), jnp.int32),
            pltpu.VMEM((2, genes, local), jnp.float32),
            pltpu.VMEM((2, per_step, genes, TILE // 2), jnp.float32),
        ],
        cost_estimate=cost(2 * perms * genes * samples * (2 * local + samples)),
        compiler_params=params(24),
        name="near",
    )(base, perm_rows, mate_rows, lead, *shards)


def reduced(best):
    perms, genes, half = best.shape
    lane = lax.broadcasted_iota(jnp.int32, (genes, half), 1)
    gene = lax.broadcasted_iota(jnp.int32, (genes, half), 0)
    rows = []
    for p in range(perms):
        top = jnp.max(best[p], axis=1, keepdims=True)
        rows.append(jnp.max(jnp.where(lane == gene, top, 0.0), axis=0, keepdims=True))
    return jnp.concatenate(rows, axis=0)


def far_kernel(start, close, table_ref, near_ref, mask_ref, one_ref, two_ref, *refs):
    genes = near_ref.shape[1]
    local = one_ref.shape[0]
    refs = list(refs)
    carried_ref = None if start else refs.pop(0)
    masks = [(mask_ref, 0), (mask_ref, 1)]
    tops = []
    for p in range(0, table_ref.shape[0] // genes, CHUNK):
        lhs = table_ref[p * genes:(p + CHUNK) * genes, :]
        best = lane_best(lhs, (one_ref, two_ref), local, masks, CHUNK)
        if not start:
            best = jnp.maximum(best, carried_ref[p:p + CHUNK])
        if close == "none":
            refs[0][p:p + CHUNK] = best
        else:
            tops.append(reduced(best))
    if close == "none":
        return
    top = jnp.maximum(jnp.concatenate(tops, axis=0), near_ref[...])
    if close == "send":
        refs[0][...] = top
        return
    mate_ref, maxima_ref, sums_ref = refs
    top = jnp.maximum(top, mate_ref[...])
    maxima = top * top * one_ref.shape[1]
    maxima_ref[...] = maxima
    log_stat = jnp.log1p(maxima)
    sums = jnp.stack((jnp.sum(log_stat, axis=0), jnp.sum(log_stat * log_stat, axis=0)))
    sums_ref[...] = jnp.broadcast_to(sums[None], sums_ref.shape)


def far_best(table, part, near, masks, pair, shards, carried=None, close="none", from_mate=None, spread=0):
    samples = table.shape[1]
    _, genes, local = masks.shape
    perms = table.shape[0] // genes // 2
    rows = perms * genes
    wide = (perms, genes, TILE // 2)
    once = pl.Buffered(1)

    def whole(shape):
        return pl.BlockSpec(shape, lambda i: (0,) * len(shape), pipeline_mode=once)

    extra = [x for x in (carried, from_mate) if x is not None]
    shape = {
        "none": [wide], "send": [(perms, genes)], "finish": [(perms, genes), (spread, 2, genes)]
    }[close]
    out = pl.pallas_call(
        functools.partial(far_kernel, carried is None, close),
        grid=(1,),
        in_specs=[
            pl.BlockSpec((rows, samples), lambda i: (part, 0), pipeline_mode=once),
            pl.BlockSpec((perms, genes), lambda i: (part, 0), pipeline_mode=once),
            pl.BlockSpec((2, genes, local), lambda i: (pair, 0, 0), pipeline_mode=once),
            whole((local, samples)),
            whole((local, samples)),
            *[whole(x.shape) for x in extra],
        ],
        out_specs=[whole(x) for x in shape],
        out_shape=[jax.ShapeDtypeStruct(x, jnp.float32) for x in shape],
        cost_estimate=cost(2 * rows * samples * 2 * local),
        compiler_params=params(24),
        name="far",
    )(table, near, masks, *shards, *extra)
    return out if len(out) > 1 else out[0]


def totals_kernel(sent_ref, moments_ref, pooled_ref):
    count, _, genes = sent_ref.shape
    blocks = lax.axis_size("gene")
    members = count // blocks
    mine = pl.multiple_of(lax.axis_index("gene") * members, members)
    moments_ref[...] = jnp.sum(sent_ref[pl.ds(mine, members)], axis=0) / PERMS
    every = jnp.sum(sent_ref[...], axis=0) / PERMS
    both = jnp.sum(every, axis=1, keepdims=True) / (genes * blocks)
    lane = lax.broadcasted_iota(jnp.int32, every.shape, 1)
    row = lax.broadcasted_iota(jnp.int32, every.shape, 0)
    spread = jnp.sum(jnp.where(lane == row, both, 0.0), axis=0, keepdims=True)
    pooled_ref[...] = spread[:, :2]


def totals(sent):
    return pl.pallas_call(
        totals_kernel,
        out_shape=[
            jax.ShapeDtypeStruct(sent.shape[1:], jnp.float32),
            jax.ShapeDtypeStruct((1, 2), jnp.float32),
        ],
        compiler_params=params(4),
        name="totals",
    )(sent)


def shards_program(genotypes, phenotypes, perm_rows, starts):
    var_n = lax.axis_size("var")
    rows_n = var_n // 2
    both = ("var", "perm")

    def along(step):
        return [(v, ((v // 2 + step) % rows_n) * 2 + v % 2) for v in range(var_n)]

    twin = [(v, v ^ 1) for v in range(var_n)]
    across = [(0, 1), (1, 0)]
    mate = [
        (v * 2 + z, ((((v // 2 + rows_n // 2) % rows_n) * 2 + v % 2) * 2 + 1 - z))
        for v in range(var_n) for z in range(2)
    ]

    mate_rows = lax.ppermute(perm_rows, both, mate)
    own, base, own_rows, lead = head(genotypes, phenotypes, perm_rows, starts)
    deep = lax.ppermute(own, "perm", across)
    below = lax.ppermute(own, "var", along(1))
    above = lax.ppermute(own, "var", along(-1))
    own_twin = lax.ppermute(own, "var", twin)
    table, near, masks = near_best(base, own_rows, mate_rows, lead, (own, own_twin))
    below, above, masks = lax.optimization_barrier((below, above, masks))
    below_twin = lax.ppermute(below, "var", twin)
    above_twin = lax.ppermute(above, "var", twin)
    lanes = far_best(table, 1, near, masks, 0, (below, above))
    deep, lanes = lax.optimization_barrier((deep, lanes))
    deep_twin = lax.ppermute(deep, "var", twin)
    lanes = far_best(table, 1, near, masks, 1, (below_twin, above_twin), lanes)
    to_mate = far_best(table, 1, near, masks, 2, (deep, deep_twin), lanes, "send")
    to_mate, masks = lax.optimization_barrier((to_mate, masks))
    from_mate = lax.ppermute(to_mate, both, mate)
    lanes = far_best(table, 0, near, masks, 0, (below, above))
    lanes = far_best(table, 0, near, masks, 1, (below_twin, above_twin), lanes)
    count = lax.axis_size(("gene", "var", "perm"))
    maxima, sums = far_best(
        table, 0, near, masks, 2, (deep, deep_twin), lanes, "finish", from_mate, count
    )

    sent = lax.all_to_all(sums, ("gene", "var", "perm"), 0, 0, tiled=True)
    moments, pooled = totals(sent)
    return (maxima, moments, pooled.reshape(2))


def solution(mesh):
    return jax.shard_map(
        shards_program,
        mesh=mesh,
        in_specs=(
            P("gene", ("var", "perm"), None),
            P("gene", None),
            P(("var", "perm"), None),
            P("gene"),
        ),
        out_specs=(P(("var", "perm"), "gene"), P(None, "gene"), P()),
        check_vma=False,
    )
```

```python
import functools

import jax
import jax.numpy as jnp
from jax import lax
from jax.experimental import pallas as pl
from jax.experimental.pallas import tpu as pltpu
from jax.sharding import PartitionSpec as P

WINDOW = 4096
PERMS = 256
FOLD = 256
TILE = 256
LARGE = 3.0e38
CHUNK = 4


def standardized(values):
    centred = values - jnp.mean(values, axis=1, keepdims=True)
    inv_norm = lax.rsqrt(jnp.sum(centred * centred, axis=1, keepdims=True) + 1.0)
    return (centred * inv_norm).astype(jnp.bfloat16)


def cost(flops):
    return pl.CostEstimate(flops=flops, bytes_accessed=0, transcendentals=0)


def places(local):
    var_n, me, z = lax.axis_size("var"), lax.axis_index("var"), lax.axis_index("perm")
    rows_n = var_n // 2
    y, core = lax.div(me, 2), lax.rem(me, 2)

    def first(up, same_core, same_depth):
        c = core if same_core else 1 - core
        d = z if same_depth else 1 - z
        return ((lax.rem(y + up + rows_n, rows_n) * 2 + c) * 2 + d) * local

    near = [first(0, True, True), first(0, False, True)]
    order = [(c, u, True) for c in (True, False) for u in (-1, 1)] + [(c, 0, False) for c in (True, False)]
    far = [first(u, c, d) for c, u, d in order]
    return near, far


def window_mask(first, lead, width):
    half = TILE // 2
    lane = lax.broadcasted_iota(jnp.int32, lead.shape, 1)
    masks = []
    for r in range(0, width, half):
        past = lane + (first + r) - lead
        masks.append(jnp.where((past >= 0) & (past < WINDOW), LARGE, 0.0))
    return jnp.concatenate(masks, axis=1)


def weight_tiles(shards, local):
    half = TILE // 2
    pieces = [(i, r) for i in range(len(shards)) for r in range(0, local, half)]
    for t in range(0, len(pieces), 2):
        pair = pieces[t:t + 2]
        yield t * half, jnp.concatenate([shards[i][r:r + half, :] for i, r in pair], axis=0)


def lane_best(rows_bf16, shards, local, masks, copies):
    half = TILE // 2
    best = None
    for at, weights in weight_tiles(shards, local):
        scores = lax.dot_general(
            rows_bf16, weights, (((1,), (1,)), ((), ())), preferred_element_type=jnp.float32
        )
        for n in range(weights.shape[0] // half):
            i, r = divmod(at + n * half, local)
            mask_ref, k = masks[i]
            mask = mask_ref[k, :, r:r + half]
            part = jnp.abs(scores[:, n * half:(n + 1) * half]).reshape(copies, mask.shape[0], half)
            part = jnp.minimum(part, mask[None])
            best = part if best is None else jnp.maximum(best, part)
    return best


def reduce_lanes(best_ref, slot, out_ref, row):
    _, perms, genes, half = best_ref.shape
    lane = lax.broadcasted_iota(jnp.int32, (genes, half), 1)
    gene = lax.broadcasted_iota(jnp.int32, (genes, half), 0)
    for p in range(perms):
        top = jnp.max(best_ref[slot, p], axis=1, keepdims=True)
        best = jnp.max(jnp.where(lane == gene, top, 0.0), axis=0, keepdims=True)
        out_ref[pl.ds(row + p, 1), :] = best


def score_step(rows_bf16, shards, local, masks, per_step, best_ref, out_ref):
    step = pl.program_id(0)
    slot = lax.rem(step, 2)
    reduce_lanes(best_ref, 1 - slot, out_ref, jnp.maximum(step - 1, 0) * per_step)
    best_ref[slot] = lane_best(rows_bf16, shards, local, masks, per_step)

    @pl.when(step == pl.num_programs(0) - 1)
    def _():
        reduce_lanes(best_ref, slot, out_ref, step * per_step)


def near_kernel(per_step, base_ref, perm_ref, mate_ref, lead_ref, own_ref, twin_ref,
                table_ref, out_ref, far_mask_ref, rows_ref, mask_ref, best_ref):
    samples = own_ref.shape[1]
    folds = samples // FOLD
    genes = base_ref.shape[0] // folds
    local = own_ref.shape[0]
    half_perms = perm_ref.shape[0]
    step = pl.program_id(0)
    near_first, far_first = places(local)

    @pl.when(step == 0)
    def _():
        rows_ref[:half_perms, :] = perm_ref[...]
        rows_ref[half_perms:, :] = mate_ref[...]
        for i in range(2):
            mask_ref[i] = window_mask(near_first[i], lead_ref[...], local)

    shard = jnp.minimum(step, len(far_first) - 1)
    first = far_first[0]
    for i in range(1, len(far_first)):
        first = jnp.where(shard == i, far_first[i], first)
    far_mask_ref[shard] = window_mask(first, lead_ref[...], local)

    within = lax.broadcasted_iota(jnp.int32, (FOLD, samples), 0)
    for k in range(per_step):
        index = rows_ref[pl.ds(step * per_step + k, 1), :]
        low = jnp.bitwise_and(index, FOLD - 1)
        block = jnp.right_shift(index, FOLD.bit_length() - 1)
        hot = jnp.where(within == low, 1.0, 0.0).astype(jnp.bfloat16)
        picked = jnp.dot(base_ref[...], hot, preferred_element_type=jnp.float32)
        chosen = picked[:genes]
        for b in range(1, folds):
            chosen = jnp.where(block == b, picked[b * genes:(b + 1) * genes], chosen)
        table_ref[k * genes:(k + 1) * genes, :] = chosen.astype(jnp.bfloat16)
    masks = [(mask_ref, 0), (mask_ref, 1)]
    score_step(table_ref[...], (own_ref, twin_ref), local, masks, per_step, best_ref, out_ref)


def params(limit):
    return pltpu.CompilerParams(vmem_limit_bytes=limit * 1024 * 1024)


def in_hbm(array):
    return pltpu.with_memory_space_constraint(array, pltpu.HBM)


def head_kernel(x_ref, pheno_ref, perm_ref, starts_ref, own_ref, base_ref, rows_ref, lead_ref):
    own_ref[...] = standardized(x_ref[0].astype(jnp.float32))
    genes, samples = pheno_ref.shape
    std = standardized(pheno_ref[...])
    for b in range(samples // FOLD):
        base_ref[b * genes:(b + 1) * genes, :] = std[:, b * FOLD:(b + 1) * FOLD]
    rows_ref[...] = perm_ref[...]
    wide = jnp.broadcast_to(starts_ref[...].astype(jnp.float32), (lead_ref.shape[1], genes))
    lead_ref[...] = wide.T.astype(jnp.int32)


def head(genotypes, phenotypes, perm_rows, starts):
    _, local, samples = genotypes.shape
    genes = phenotypes.shape[0]
    inputs = (genotypes, phenotypes, perm_rows, starts.reshape(1, genes))
    return pl.pallas_call(
        head_kernel,
        out_shape=[
            jax.ShapeDtypeStruct((local, samples), jnp.bfloat16),
            jax.ShapeDtypeStruct((samples // FOLD * genes, FOLD), jnp.bfloat16),
            jax.ShapeDtypeStruct(perm_rows.shape, jnp.int32),
            jax.ShapeDtypeStruct((genes, TILE // 2), jnp.int32),
        ],
        cost_estimate=cost(8 * local * samples),
        compiler_params=params(16),
        name="head",
    )(*(in_hbm(i) for i in inputs))


def near_best(base, perm_rows, mate_rows, lead, shards):
    genes, samples = lead.shape[0], shards[0].shape[1]
    perms = perm_rows.shape[0] + mate_rows.shape[0]
    local = shards[0].shape[0]
    per_step = 4
    once = pl.Buffered(1)

    def whole(shape):
        return pl.BlockSpec(shape, lambda i: (0, 0), pipeline_mode=once)

    return pl.pallas_call(
        functools.partial(near_kernel, per_step),
        grid=(perms // per_step,),
        in_specs=[
            whole(base.shape),
            whole(perm_rows.shape),
            whole(mate_rows.shape),
            whole(lead.shape),
            whole((local, samples)),
            whole((local, samples)),
        ],
        out_specs=[
            pl.BlockSpec((per_step * genes, samples), lambda i: (i, 0)),
            pl.BlockSpec((perms, genes), lambda i: (0, 0)),
            pl.BlockSpec((6, genes, local), lambda i: (0, 0, 0)),
        ],
        out_shape=[
            jax.ShapeDtypeStruct((perms * genes, samples), jnp.bfloat16),
            jax.ShapeDtypeStruct((perms, genes), jnp.float32),
            jax.ShapeDtypeStruct((6, genes, local), jnp.float32),
        ],
        scratch_shapes=[
            pltpu.VMEM((perms, samples), jnp.int32),
            pltpu.VMEM((2, genes, local), jnp.float32),
            pltpu.VMEM((2, per_step, genes, TILE // 2), jnp.float32),
        ],
        cost_estimate=cost(2 * perms * genes * samples * (2 * local + samples)),
        compiler_params=params(24),
        name="near",
    )(base, perm_rows, mate_rows, lead, *shards)


def reduced(best):
    perms, genes, half = best.shape
    lane = lax.broadcasted_iota(jnp.int32, (genes, half), 1)
    gene = lax.broadcasted_iota(jnp.int32, (genes, half), 0)
    rows = []
    for p in range(perms):
        top = jnp.max(best[p], axis=1, keepdims=True)
        rows.append(jnp.max(jnp.where(lane == gene, top, 0.0), axis=0, keepdims=True))
    return jnp.concatenate(rows, axis=0)


def far_kernel(start, close, pairs, table_ref, near_ref, *refs):
    genes = near_ref.shape[1]
    mask_refs, shards, refs = refs[:pairs], refs[pairs:3 * pairs], refs[3 * pairs:]
    local, samples = shards[0].shape
    refs = list(refs)
    carried_ref = None if start else refs.pop(0)
    masks = [(m, k) for m in mask_refs for k in range(2)]
    tops = []
    for p in range(0, table_ref.shape[0] // genes, CHUNK):
        lhs = table_ref[p * genes:(p + CHUNK) * genes, :]
        best = lane_best(lhs, shards, local, masks, CHUNK)
        if not start:
            best = jnp.maximum(best, carried_ref[p:p + CHUNK])
        if close == "none":
            refs[0][p:p + CHUNK] = best
        else:
            tops.append(reduced(best))
    if close == "none":
        return
    top = jnp.maximum(jnp.concatenate(tops, axis=0), near_ref[...])
    if close == "send":
        refs[0][...] = top
        return
    mate_ref, maxima_ref, sums_ref = refs
    top = jnp.maximum(top, mate_ref[...])
    maxima = top * top * samples
    maxima_ref[...] = maxima
    log_stat = jnp.log1p(maxima)
    sums = jnp.stack((jnp.sum(log_stat, axis=0), jnp.sum(log_stat * log_stat, axis=0)))
    sums_ref[...] = jnp.broadcast_to(sums[None], sums_ref.shape)


def far_best(table, part, near, masks, pairs, shards, carried=None, close="none", from_mate=None, spread=0):
    samples = table.shape[1]
    _, genes, local = masks.shape
    perms = table.shape[0] // genes // 2
    rows = perms * genes
    wide = (perms, genes, TILE // 2)
    once = pl.Buffered(1)

    def whole(shape):
        return pl.BlockSpec(shape, lambda i: (0,) * len(shape), pipeline_mode=once)

    extra = [x for x in (carried, from_mate) if x is not None]
    shape = {
        "none": [wide], "send": [(perms, genes)], "finish": [(perms, genes), (spread, 2, genes)]
    }[close]
    out = pl.pallas_call(
        functools.partial(far_kernel, carried is None, close, len(pairs)),
        grid=(1,),
        in_specs=[
            pl.BlockSpec((rows, samples), lambda i: (part, 0), pipeline_mode=once),
            pl.BlockSpec((perms, genes), lambda i: (part, 0), pipeline_mode=once),
            *[pl.BlockSpec((2, genes, local), lambda i, k=k: (k, 0, 0), pipeline_mode=once) for k in pairs],
            *[whole((local, samples))] * len(shards),
            *[whole(x.shape) for x in extra],
        ],
        out_specs=[whole(x) for x in shape],
        out_shape=[jax.ShapeDtypeStruct(x, jnp.float32) for x in shape],
        cost_estimate=cost(2 * rows * samples * len(shards) * local),
        compiler_params=params(24),
        name="far",
    )(table, near, *[masks] * len(pairs), *shards, *extra)
    return out if len(out) > 1 else out[0]


def totals_kernel(sent_ref, moments_ref, pooled_ref):
    count, _, genes = sent_ref.shape
    blocks = lax.axis_size("gene")
    members = count // blocks
    mine = pl.multiple_of(lax.axis_index("gene") * members, members)
    moments_ref[...] = jnp.sum(sent_ref[pl.ds(mine, members)], axis=0) / PERMS
    every = jnp.sum(sent_ref[...], axis=0) / PERMS
    both = jnp.sum(every, axis=1, keepdims=True) / (genes * blocks)
    lane = lax.broadcasted_iota(jnp.int32, every.shape, 1)
    row = lax.broadcasted_iota(jnp.int32, every.shape, 0)
    spread = jnp.sum(jnp.where(lane == row, both, 0.0), axis=0, keepdims=True)
    pooled_ref[...] = spread[:, :2]


def totals(sent):
    return pl.pallas_call(
        totals_kernel,
        out_shape=[
            jax.ShapeDtypeStruct(sent.shape[1:], jnp.float32),
            jax.ShapeDtypeStruct((1, 2), jnp.float32),
        ],
        compiler_params=params(4),
        name="totals",
    )(sent)


def shards_program(genotypes, phenotypes, perm_rows, starts):
    var_n = lax.axis_size("var")
    rows_n = var_n // 2
    both = ("var", "perm")

    def along(step):
        return [(v, ((v // 2 + step) % rows_n) * 2 + v % 2) for v in range(var_n)]

    twin = [(v, v ^ 1) for v in range(var_n)]
    across = [(0, 1), (1, 0)]
    mate = [
        (v * 2 + z, ((((v // 2 + rows_n // 2) % rows_n) * 2 + v % 2) * 2 + 1 - z))
        for v in range(var_n) for z in range(2)
    ]

    mate_rows = lax.ppermute(perm_rows, both, mate)
    own, base, own_rows, lead = head(genotypes, phenotypes, perm_rows, starts)
    deep = lax.ppermute(own, "perm", across)
    below = lax.ppermute(own, "var", along(1))
    above = lax.ppermute(own, "var", along(-1))
    own_twin = lax.ppermute(own, "var", twin)
    table, near, masks = near_best(base, own_rows, mate_rows, lead, (own, own_twin))
    below, above, masks = lax.optimization_barrier((below, above, masks))
    below_twin = lax.ppermute(below, "var", twin)
    above_twin = lax.ppermute(above, "var", twin)
    lanes = far_best(table, 1, near, masks, (0,), (below, above))
    deep, lanes = lax.optimization_barrier((deep, lanes))
    deep_twin = lax.ppermute(deep, "var", twin)
    lanes = far_best(table, 1, near, masks, (1,), (below_twin, above_twin), lanes)
    to_mate = far_best(table, 1, near, masks, (2,), (deep, deep_twin), lanes, "send")
    from_mate = lax.ppermute(to_mate, both, mate)
    lanes = far_best(table, 0, near, masks, (0, 1), (below, above, below_twin, above_twin))
    count = lax.axis_size(("gene", "var", "perm"))
    maxima, sums = far_best(
        table, 0, near, masks, (2,), (deep, deep_twin), lanes, "finish", from_mate, count
    )

    sent = lax.all_to_all(sums, ("gene", "var", "perm"), 0, 0, tiled=True)
    moments, pooled = totals(sent)
    return (maxima, moments, pooled.reshape(2))


def solution(mesh):
    return jax.shard_map(
        shards_program,
        mesh=mesh,
        in_specs=(
            P("gene", ("var", "perm"), None),
            P("gene", None),
            P(("var", "perm"), None),
            P("gene"),
        ),
        out_specs=(P(("var", "perm"), "gene"), P(None, "gene"), P()),
        check_vma=False,
    )
```

```python
import functools

import jax
import jax.numpy as jnp
from jax import lax
from jax.experimental import pallas as pl
from jax.experimental.pallas import tpu as pltpu
from jax.sharding import PartitionSpec as P

WINDOW = 4096
PERMS = 256
FOLD = 256
TILE = 256
LARGE = 3.0e38
CHUNK = 8


def standardized(values):
    centred = values - jnp.mean(values, axis=1, keepdims=True)
    inv_norm = lax.rsqrt(jnp.sum(centred * centred, axis=1, keepdims=True) + 1.0)
    return (centred * inv_norm).astype(jnp.bfloat16)


def cost(flops):
    return pl.CostEstimate(flops=flops, bytes_accessed=0, transcendentals=0)


def places(local):
    var_n, me, z = lax.axis_size("var"), lax.axis_index("var"), lax.axis_index("perm")
    rows_n = var_n // 2
    y, core = lax.div(me, 2), lax.rem(me, 2)

    def first(up, same_core, same_depth):
        c = core if same_core else 1 - core
        d = z if same_depth else 1 - z
        return ((lax.rem(y + up + rows_n, rows_n) * 2 + c) * 2 + d) * local

    near = [first(0, True, True), first(0, False, True)]
    order = [(c, u, True) for c in (True, False) for u in (-1, 1)] + [(c, 0, False) for c in (True, False)]
    far = [first(u, c, d) for c, u, d in order]
    return near, far


def window_mask(first, lead, width):
    half = TILE // 2
    lane = lax.broadcasted_iota(jnp.int32, lead.shape, 1)
    masks = []
    for r in range(0, width, half):
        past = lane + (first + r) - lead
        masks.append(jnp.where((past >= 0) & (past < WINDOW), LARGE, 0.0))
    return jnp.concatenate(masks, axis=1)


def weight_tiles(shards, local):
    half = TILE // 2
    pieces = [(i, r) for i in range(len(shards)) for r in range(0, local, half)]
    for t in range(0, len(pieces), 2):
        pair = pieces[t:t + 2]
        yield t * half, jnp.concatenate([shards[i][r:r + half, :] for i, r in pair], axis=0)


def lane_best(rows_bf16, shards, local, masks, copies):
    half = TILE // 2
    best = None
    for at, weights in weight_tiles(shards, local):
        scores = lax.dot_general(
            rows_bf16, weights, (((1,), (1,)), ((), ())), preferred_element_type=jnp.float32
        )
        for n in range(weights.shape[0] // half):
            i, r = divmod(at + n * half, local)
            mask_ref, k = masks[i]
            mask = mask_ref[k, :, r:r + half]
            part = jnp.abs(scores[:, n * half:(n + 1) * half]).reshape(copies, mask.shape[0], half)
            part = jnp.minimum(part, mask[None])
            best = part if best is None else jnp.maximum(best, part)
    return best


def reduce_lanes(best_ref, slot, out_ref, row):
    _, perms, genes, half = best_ref.shape
    lane = lax.broadcasted_iota(jnp.int32, (genes, half), 1)
    gene = lax.broadcasted_iota(jnp.int32, (genes, half), 0)
    for p in range(perms):
        top = jnp.max(best_ref[slot, p], axis=1, keepdims=True)
        best = jnp.max(jnp.where(lane == gene, top, 0.0), axis=0, keepdims=True)
        out_ref[pl.ds(row + p, 1), :] = best


def score_step(rows_bf16, shards, local, masks, per_step, best_ref, out_ref):
    step = pl.program_id(0)
    slot = lax.rem(step, 2)
    reduce_lanes(best_ref, 1 - slot, out_ref, jnp.maximum(step - 1, 0) * per_step)
    best_ref[slot] = lane_best(rows_bf16, shards, local, masks, per_step)

    @pl.when(step == pl.num_programs(0) - 1)
    def _():
        reduce_lanes(best_ref, slot, out_ref, step * per_step)


def near_kernel(per_step, base_ref, perm_ref, mate_ref, lead_ref, own_ref, twin_ref,
                table_ref, out_ref, far_mask_ref, rows_ref, mask_ref, best_ref):
    samples = own_ref.shape[1]
    folds = samples // FOLD
    genes = base_ref.shape[0] // folds
    local = own_ref.shape[0]
    half_perms = perm_ref.shape[0]
    step = pl.program_id(0)
    near_first, far_first = places(local)

    @pl.when(step == 0)
    def _():
        rows_ref[:half_perms, :] = perm_ref[...]
        rows_ref[half_perms:, :] = mate_ref[...]
        for i in range(2):
            mask_ref[i] = window_mask(near_first[i], lead_ref[...], local)

    shard = jnp.minimum(step, len(far_first) - 1)
    first = far_first[0]
    for i in range(1, len(far_first)):
        first = jnp.where(shard == i, far_first[i], first)
    far_mask_ref[shard] = window_mask(first, lead_ref[...], local)

    within = lax.broadcasted_iota(jnp.int32, (FOLD, samples), 0)
    for k in range(per_step):
        index = rows_ref[pl.ds(step * per_step + k, 1), :]
        low = jnp.bitwise_and(index, FOLD - 1)
        block = jnp.right_shift(index, FOLD.bit_length() - 1)
        hot = jnp.where(within == low, 1.0, 0.0).astype(jnp.bfloat16)
        picked = jnp.dot(base_ref[...], hot, preferred_element_type=jnp.float32)
        chosen = picked[:genes]
        for b in range(1, folds):
            chosen = jnp.where(block == b, picked[b * genes:(b + 1) * genes], chosen)
        table_ref[k * genes:(k + 1) * genes, :] = chosen.astype(jnp.bfloat16)
    masks = [(mask_ref, 0), (mask_ref, 1)]
    score_step(table_ref[...], (own_ref, twin_ref), local, masks, per_step, best_ref, out_ref)


def params(limit):
    return pltpu.CompilerParams(vmem_limit_bytes=limit * 1024 * 1024)


def in_hbm(array):
    return pltpu.with_memory_space_constraint(array, pltpu.HBM)


def head_kernel(x_ref, pheno_ref, perm_ref, starts_ref, own_ref, base_ref, rows_ref, lead_ref):
    own_ref[...] = standardized(x_ref[0].astype(jnp.float32))
    genes, samples = pheno_ref.shape
    std = standardized(pheno_ref[...])
    for b in range(samples // FOLD):
        base_ref[b * genes:(b + 1) * genes, :] = std[:, b * FOLD:(b + 1) * FOLD]
    rows_ref[...] = perm_ref[...]
    wide = jnp.broadcast_to(starts_ref[...].astype(jnp.float32), (lead_ref.shape[1], genes))
    lead_ref[...] = wide.T.astype(jnp.int32)


def head(genotypes, phenotypes, perm_rows, starts):
    _, local, samples = genotypes.shape
    genes = phenotypes.shape[0]
    inputs = (genotypes, phenotypes, perm_rows, starts.reshape(1, genes))
    return pl.pallas_call(
        head_kernel,
        out_shape=[
            jax.ShapeDtypeStruct((local, samples), jnp.bfloat16),
            jax.ShapeDtypeStruct((samples // FOLD * genes, FOLD), jnp.bfloat16),
            jax.ShapeDtypeStruct(perm_rows.shape, jnp.int32),
            jax.ShapeDtypeStruct((genes, TILE // 2), jnp.int32),
        ],
        cost_estimate=cost(8 * local * samples),
        compiler_params=params(16),
        name="head",
    )(*(in_hbm(i) for i in inputs))


def near_best(base, perm_rows, mate_rows, lead, shards):
    genes, samples = lead.shape[0], shards[0].shape[1]
    perms = perm_rows.shape[0] + mate_rows.shape[0]
    local = shards[0].shape[0]
    per_step = 4
    once = pl.Buffered(1)

    def whole(shape):
        return pl.BlockSpec(shape, lambda i: (0, 0), pipeline_mode=once)

    return pl.pallas_call(
        functools.partial(near_kernel, per_step),
        grid=(perms // per_step,),
        in_specs=[
            whole(base.shape),
            whole(perm_rows.shape),
            whole(mate_rows.shape),
            whole(lead.shape),
            whole((local, samples)),
            whole((local, samples)),
        ],
        out_specs=[
            pl.BlockSpec((per_step * genes, samples), lambda i: (i, 0)),
            pl.BlockSpec((perms, genes), lambda i: (0, 0)),
            pl.BlockSpec((6, genes, local), lambda i: (0, 0, 0)),
        ],
        out_shape=[
            jax.ShapeDtypeStruct((perms * genes, samples), jnp.bfloat16),
            jax.ShapeDtypeStruct((perms, genes), jnp.float32),
            jax.ShapeDtypeStruct((6, genes, local), jnp.float32),
        ],
        scratch_shapes=[
            pltpu.VMEM((perms, samples), jnp.int32),
            pltpu.VMEM((2, genes, local), jnp.float32),
            pltpu.VMEM((2, per_step, genes, TILE // 2), jnp.float32),
        ],
        cost_estimate=cost(2 * perms * genes * samples * (2 * local + samples)),
        compiler_params=params(24),
        name="near",
    )(base, perm_rows, mate_rows, lead, *shards)


def reduced(best):
    perms, genes, half = best.shape
    lane = lax.broadcasted_iota(jnp.int32, (genes, half), 1)
    gene = lax.broadcasted_iota(jnp.int32, (genes, half), 0)
    rows = []
    for p in range(perms):
        top = jnp.max(best[p], axis=1, keepdims=True)
        rows.append(jnp.max(jnp.where(lane == gene, top, 0.0), axis=0, keepdims=True))
    return jnp.concatenate(rows, axis=0)


def far_kernel(start, close, pairs, table_ref, near_ref, *refs):
    genes = near_ref.shape[1]
    mask_refs, shards, refs = refs[:pairs], refs[pairs:3 * pairs], refs[3 * pairs:]
    local, samples = shards[0].shape
    refs = list(refs)
    carried_ref = None if start else refs.pop(0)
    masks = [(m, k) for m in mask_refs for k in range(2)]
    tops = []
    for p in range(0, table_ref.shape[0] // genes, CHUNK):
        lhs = table_ref[p * genes:(p + CHUNK) * genes, :]
        best = lane_best(lhs, shards, local, masks, CHUNK)
        if not start:
            best = jnp.maximum(best, carried_ref[p:p + CHUNK])
        if close == "none":
            refs[0][p:p + CHUNK] = best
        else:
            tops.append(reduced(best))
    if close == "none":
        return
    top = jnp.maximum(jnp.concatenate(tops, axis=0), near_ref[...])
    if close == "send":
        refs[0][...] = top
        return
    mate_ref, maxima_ref, sums_ref = refs
    top = jnp.maximum(top, mate_ref[...])
    maxima = top * top * samples
    maxima_ref[...] = maxima
    log_stat = jnp.log1p(maxima)
    sums = jnp.stack((jnp.sum(log_stat, axis=0), jnp.sum(log_stat * log_stat, axis=0)))
    sums_ref[...] = jnp.broadcast_to(sums[None], sums_ref.shape)


def far_best(table, part, near, masks, pairs, shards, carried=None, close="none", from_mate=None, spread=0):
    samples = table.shape[1]
    _, genes, local = masks.shape
    perms = table.shape[0] // genes // 2
    rows = perms * genes
    wide = (perms, genes, TILE // 2)
    once = pl.Buffered(1)

    def whole(shape):
        return pl.BlockSpec(shape, lambda i: (0,) * len(shape), pipeline_mode=once)

    extra = [x for x in (carried, from_mate) if x is not None]
    shape = {
        "none": [wide], "send": [(perms, genes)], "finish": [(perms, genes), (spread, 2, genes)]
    }[close]
    out = pl.pallas_call(
        functools.partial(far_kernel, carried is None, close, len(pairs)),
        grid=(1,),
        in_specs=[
            pl.BlockSpec((rows, samples), lambda i: (part, 0), pipeline_mode=once),
            pl.BlockSpec((perms, genes), lambda i: (part, 0), pipeline_mode=once),
            *[pl.BlockSpec((2, genes, local), lambda i, k=k: (k, 0, 0), pipeline_mode=once) for k in pairs],
            *[whole((local, samples))] * len(shards),
            *[whole(x.shape) for x in extra],
        ],
        out_specs=[whole(x) for x in shape],
        out_shape=[jax.ShapeDtypeStruct(x, jnp.float32) for x in shape],
        cost_estimate=cost(2 * rows * samples * len(shards) * local),
        compiler_params=params(24),
        name="far",
    )(table, near, *[masks] * len(pairs), *shards, *extra)
    return out if len(out) > 1 else out[0]


def totals_kernel(sent_ref, held_ref, maxima_ref, moments_ref, pooled_ref):
    maxima_ref[...] = held_ref[...]
    count, _, genes = sent_ref.shape
    blocks = lax.axis_size("gene")
    members = count // blocks
    mine = pl.multiple_of(lax.axis_index("gene") * members, members)
    moments_ref[...] = jnp.sum(sent_ref[pl.ds(mine, members)], axis=0) / PERMS
    every = jnp.sum(sent_ref[...], axis=0) / PERMS
    both = jnp.sum(every, axis=1, keepdims=True) / (genes * blocks)
    lane = lax.broadcasted_iota(jnp.int32, every.shape, 1)
    row = lax.broadcasted_iota(jnp.int32, every.shape, 0)
    spread = jnp.sum(jnp.where(lane == row, both, 0.0), axis=0, keepdims=True)
    pooled_ref[...] = spread[:, :2]


def totals(sent, held):
    return pl.pallas_call(
        totals_kernel,
        out_shape=[
            jax.ShapeDtypeStruct(held.shape, jnp.float32),
            jax.ShapeDtypeStruct(sent.shape[1:], jnp.float32),
            jax.ShapeDtypeStruct((1, 2), jnp.float32),
        ],
        compiler_params=params(4),
        name="totals",
    )(sent, held)


def shards_program(genotypes, phenotypes, perm_rows, starts):
    var_n = lax.axis_size("var")
    rows_n = var_n // 2
    both = ("var", "perm")

    def along(step):
        return [(v, ((v // 2 + step) % rows_n) * 2 + v % 2) for v in range(var_n)]

    twin = [(v, v ^ 1) for v in range(var_n)]
    across = [(0, 1), (1, 0)]
    mate = [
        (v * 2 + z, ((((v // 2 + rows_n // 2) % rows_n) * 2 + v % 2) * 2 + 1 - z))
        for v in range(var_n) for z in range(2)
    ]

    mate_rows = lax.ppermute(perm_rows, both, mate)
    own, base, own_rows, lead = head(genotypes, phenotypes, perm_rows, starts)
    deep = lax.ppermute(own, "perm", across)
    below = lax.ppermute(own, "var", along(1))
    above = lax.ppermute(own, "var", along(-1))
    own_twin = lax.ppermute(own, "var", twin)
    table, near, masks = near_best(base, own_rows, mate_rows, lead, (own, own_twin))
    below, above, masks = lax.optimization_barrier((below, above, masks))
    below_twin = lax.ppermute(below, "var", twin)
    above_twin = lax.ppermute(above, "var", twin)
    lanes = far_best(table, 1, near, masks, (0,), (below, above))
    deep, lanes = lax.optimization_barrier((deep, lanes))
    deep_twin = lax.ppermute(deep, "var", twin)
    lanes = far_best(table, 1, near, masks, (1,), (below_twin, above_twin), lanes)
    to_mate = far_best(table, 1, near, masks, (2,), (deep, deep_twin), lanes, "send")
    from_mate = lax.ppermute(to_mate, both, mate)
    lanes = far_best(table, 0, near, masks, (0, 1), (below, above, below_twin, above_twin))
    count = lax.axis_size(("gene", "var", "perm"))
    held, sums = far_best(
        table, 0, near, masks, (2,), (deep, deep_twin), lanes, "finish", from_mate, count
    )

    sent = lax.all_to_all(sums, ("gene", "var", "perm"), 0, 0, tiled=True)
    maxima, moments, pooled = totals(sent, held)
    return (maxima, moments, pooled.reshape(2))


def solution(mesh):
    return jax.shard_map(
        shards_program,
        mesh=mesh,
        in_specs=(
            P("gene", ("var", "perm"), None),
            P("gene", None),
            P(("var", "perm"), None),
            P("gene"),
        ),
        out_specs=(P(("var", "perm"), "gene"), P(None, "gene"), P()),
        check_vma=False,
    )
```
